128 devices in a mesh: dp: 8 (over y, core), mp: 16 (over x, z).
Axes of the slice: x: 4, y: 4, z: 4, core: 2. Of those that a mesh axis runs over, the one named last changes fastest.
Arguments:
- layer_input: bfloat16 [256, 256, 768], P(('dp', 'mp')), may hold values from -6 to 6
- output_cot: bfloat16 [256, 256, 768], P(('dp', 'mp')), may hold values from -6 to 6
- hidden_act: bfloat16 [256, 3072, 256], P('dp', 'mp'), may hold values from 0 to 2
- hidden_cot: bfloat16 [256, 3072, 256], P('dp', 'mp'), may hold values from -6 to 6
- lengths: int32 [256], P('dp'), may hold values from 32 to 256
- weights: float32 [768, 6144], P('dp', 'mp'), may hold values from -0.21875 to 0.21875
- moment_one: float32 [768, 6144], P('dp', 'mp'), may hold values from -3 to 3
- moment_two: float32 [768, 6144], P('dp', 'mp'), may hold values from 0.0005 to 0.02
Outputs:
- new_weights: float32 [768, 6144], P('dp', 'mp')
- new_moment_one: float32 [768, 6144], P('dp', 'mp')
- new_moment_two: float32 [768, 6144], P('dp', 'mp')
- clip_scale: float32 [256], P('dp')
The draws below stay inside these ranges and needn't reach their ends.
Inputs may be any that keep to these rules, and one draw needn't show every extreme that they name: `lengths`: slots from an example's length on are padding.
All inputs are finite; a program needn't handle non-finite values.
Results may differ from the reference program's by a relative error of at most 0.0024.
Values may be sent and summed in bfloat16 or wider, within the bound.
A program may use at most 128 MiB of HBM per device.

```python
import math
import jax
import jax.numpy as jnp
from jax import lax

D = 768
FF = 3072
SLOT = 256
STEP = 10
EXAMPLES = 256


def set_ends(values, own_key, least, top_value):
    longest = values.shape.index(max(values.shape))
    spots = []
    for shift in (0, 1):
        where = [jax.random.randint(jax.random.fold_in(own_key, axis), (), 0, length) for axis, length in enumerate(values.shape)]
        where[longest] = (where[longest] + shift) % values.shape[longest]
        spots.append(tuple(where))
    return values.at[spots[0]].set(least).at[spots[1]].set(top_value)


def steps_of(stream_key, dims, shards, least, high):
    loudness = 1.0
    for position, blocks in shards:
        heights = jax.random.uniform(jax.random.fold_in(jax.random.fold_in(stream_key, 6), position), (blocks,), jnp.float32, least / len(shards), high / len(shards))
        loudness = loudness * jnp.repeat(jnp.exp(heights), dims[position] // blocks).reshape((-1,) + (1,) * (len(dims) - 1 - position))
    return loudness


def gaussian(rng, shape, deviation, bound, split=(), kind=jnp.bfloat16):
    gain = steps_of(rng, shape, split, -0.22, 0.18) if split else 1.0
    values = jax.random.normal(rng, shape, jnp.float32) * deviation * gain
    return jnp.minimum(jnp.maximum(values, -bound), bound).astype(kind)


def setup_inputs(seed: int = 0) -> dict:
    key_of = jax.random.split(jax.random.key(seed), 9)
    return {
        "layer_input": gaussian(key_of[0], (EXAMPLES, SLOT, D), 1.0, 6.0, ((0, 128),)),
        "output_cot": gaussian(key_of[1], (EXAMPLES, SLOT, D), 1.0, 6.0, ((0, 128),)),
        "hidden_act": jnp.clip(2.0 * jax.random.uniform(key_of[2], (EXAMPLES, FF, SLOT), jnp.float32) ** steps_of(key_of[2], (EXAMPLES, FF, SLOT), ((0, 8), (1, 16)), -0.2, 0.2), 0.0, 2.0).astype(jnp.bfloat16),
        "hidden_cot": gaussian(key_of[3], (EXAMPLES, FF, SLOT), 1.0, 6.0, ((0, 8), (1, 16))),
        "lengths": set_ends(jax.random.randint(key_of[4], (EXAMPLES,), SLOT // 8, SLOT + 1), jax.random.fold_in(key_of[4], 1), SLOT // 8, SLOT).astype(jnp.int32),
        "weights": gaussian(key_of[5], (D, 2 * FF), D ** -0.5, 0.21875, ((0, 8), (1, 16)), jnp.float32),
        "moment_one": gaussian(key_of[6], (D, 2 * FF), 0.5, 3.0, ((0, 8), (1, 16)), jnp.float32),
        "moment_two": jnp.clip(jnp.exp(math.log(0.02) - 3.6888794 * jax.random.uniform(key_of[7], (D, 2 * FF), jnp.float32) ** steps_of(key_of[7], (D, 2 * FF), ((0, 8), (1, 16)), -0.2, 0.2)), 0.0005, 0.02),
    }


beta_one = 0.9
beta_two = 0.999
adam_eps = 1e-08
learn_rate = 0.001
weight_decay = 0.01

def pair_norm(example_items):
    input_rows, outcot_rows, cot_rows, hid_rows = example_items
    input_gram = jnp.dot(input_rows, input_rows.T, preferred_element_type=jnp.float32)
    cot_gram = jnp.dot(cot_rows.T, cot_rows, preferred_element_type=jnp.float32)
    outcot_gram = jnp.dot(outcot_rows, outcot_rows.T, preferred_element_type=jnp.float32)
    hid_gram = jnp.dot(hid_rows.T, hid_rows, preferred_element_type=jnp.float32)
    return jnp.sum(input_gram * cot_gram) + jnp.sum(outcot_gram * hid_gram)

def reference(layer_input, output_cot, hidden_act, hidden_cot, lengths, weights, moment_one, moment_two):
    slot_index = lax.broadcasted_iota(jnp.int32, (EXAMPLES, SLOT), 1)
    token_mask = (slot_index < lengths[:, None].astype(jnp.int32)).astype(jnp.float32)
    cot_masked = (hidden_cot.astype(jnp.float32) * token_mask[:, None, :]).astype(jnp.bfloat16)
    hid_masked = (hidden_act.astype(jnp.float32) * token_mask[:, None, :]).astype(jnp.bfloat16)
    squares = lax.map(pair_norm, (layer_input, output_cot, cot_masked, hid_masked))
    clip_limit = 0.5 * math.sqrt(2.0 * D * FF * SLOT)
    clip_scale = clip_limit / jnp.maximum(jnp.sqrt(squares), clip_limit)
    factor = clip_scale[:, None] * token_mask
    scaled_cot = (hidden_cot.astype(jnp.float32) * factor[:, None, :]).astype(jnp.bfloat16)
    scaled_hid = (hidden_act.astype(jnp.float32) * factor[:, None, :]).astype(jnp.bfloat16)
    contract = (((0, 1), (0, 2)), ((), ()))
    first_part = lax.dot_general(layer_input, scaled_cot, contract, preferred_element_type=jnp.float32)
    second_part = lax.dot_general(output_cot, scaled_hid, contract, preferred_element_type=jnp.float32)
    gradient = jnp.stack([first_part, second_part], axis=2).reshape(D, 2 * FF) / EXAMPLES
    new_moment_one = beta_one * moment_one + (1.0 - beta_one) * gradient
    new_moment_two = beta_two * moment_two + (1.0 - beta_two) * gradient * gradient
    corr_one = 1.0 - beta_one ** STEP
    corr_two = 1.0 - beta_two ** STEP
    direction = new_moment_one / corr_one / (jnp.sqrt(new_moment_two / corr_two) + adam_eps)
    new_weights = weights - learn_rate * (direction + weight_decay * weights)
    return (new_weights, new_moment_one, new_moment_two, clip_scale)
```

```python
import math

import jax
import jax.numpy as jnp
from jax import lax
from jax.experimental import pallas as pl
from jax.experimental.pallas import tpu as pltpu
from jax.sharding import PartitionSpec as P

D = 768
FF = 3072
SLOT = 256
STEP = 10
EXAMPLES = 256
ROWS = 192
OWN = 96

beta_one = 0.9
beta_two = 0.999
adam_eps = 1e-08
learn_rate = 0.001
weight_decay = 0.01
clip_limit = 0.5 * math.sqrt(2.0 * D * FF * SLOT)

MESH = pl.DeviceIdType.MESH
BF16 = jnp.bfloat16
F32 = jnp.float32


def kernel(
    x0_ref, x1_ref, h0_ref, h1_ref, len_ref,
    grad_ref, clip_ref,
    xb, hb, rb, gacc, gs, gr, gpad, ys, yr, eb, lb, mt, ft, npart, nb,
    lsem, llen, sx, sxo, sr, sh, sho, slen, sxf, srf, sn, sg, sy,
    rx, rxo, rr, rh, rho, rlen, rn, rg, ry,
):
    dp, mp = lax.axis_index("dp"), lax.axis_index("mp")
    c, y = lax.rem(dp, 2), lax.div(dp, 2)
    x, z = lax.div(mp, 4), lax.rem(mp, 4)
    other = 1 - c
    mod4 = lambda v: lax.rem(v + 8, 4)
    g = c * z + (1 - c) * x
    a = c * x + (1 - c) * z
    mp_of = lambda gg, aa: (1 - c) * (gg * 4 + aa) + c * (aa * 4 + gg)

    def remote(src, dst, ssem, rsem, to_dp, to_mp):
        return pltpu.make_async_remote_copy(
            src_ref=src, dst_ref=dst, send_sem=ssem, recv_sem=rsem,
            device_id={"dp": to_dp, "mp": to_mp}, device_id_type=MESH,
        )

    x_refs, h_refs = (x0_ref, x1_ref), (h0_ref, h1_ref)
    SIGN = (1, -1)
    OFF = (0, 1, 3, 2)
    HALF = ((0, 1), (3, 2))

    def place(k):
        return (x, z) if k == 0 else (z, x)

    def mp_k(k, gg, aa):
        return gg * 4 + aa if k == 0 else aa * 4 + gg

    def h_slice(k, i, aa):
        return h_refs[k].at[i, aa] if k == 0 else h_refs[k].at[aa, i]

    def h_all(k, aa):
        return h_refs[k].at[:, aa] if k == 0 else h_refs[k].at[aa]

    def d_x(k, s, j):
        gk, ak = place(k)
        return remote(x_refs[k].at[j], xb.at[c, gk, j], sx.at[k, s, j], rx.at[c, s, j],
                      y * 2 + k, mp_k(k, mod4(gk + SIGN[s]), ak))

    def d_relay(k, s, n):
        gk, ak = place(k)
        i = mod4(gk + HALF[s][n])
        return remote(h_slice(k, i, mod4(ak + 2)), rb.at[c, s, n], sr.at[k, s, n], rr.at[c, s, n],
                      y * 2 + k, mp_k(k, gk, mod4(ak + SIGN[s])))

    def d_h(k, s, n):
        gk, ak = place(k)
        i = mod4(gk + OFF[n])
        aa = mod4(ak + SIGN[s])
        return remote(h_slice(k, i, aa), hb.at[c, i, :, ak], sh.at[k, s, n], rh.at[c, s, n],
                      y * 2 + k, mp_k(k, gk, aa))

    def d_own_remote(k):
        gk, ak = place(k)
        return (
            remote(x_refs[k], xb.at[c, gk], sxo, rxo, y * 2 + k, mp),
            remote(h_all(k, ak), hb.at[c, :, :, ak], sho, rho, y * 2 + k, mp),
        )

    def d_own_local(k):
        gk, ak = place(k)
        return (
            pltpu.make_async_copy(x_refs[k], xb.at[c, gk], lsem.at[0]),
            pltpu.make_async_copy(h_all(k, ak), hb.at[c, :, :, ak], lsem.at[1]),
        )

    d_len = remote(len_ref, lb.at[c], slen, rlen, y * 2 + other, mp)
    d_len_local = pltpu.make_async_copy(len_ref, lb.at[c], llen)

    def d_xf(cp, s):
        src = xb.at[cp, mod4(g - SIGN[s]), s]
        return remote(src, src, sxf.at[cp, s], rx.at[cp, 2, s], dp, mp_of(mod4(g + SIGN[s]), a))

    def d_rf(cp, s, n):
        i = mod4(g + HALF[s][n])
        return remote(rb.at[cp, s, n], hb.at[cp, i, :, mod4(a - SIGN[s])], srf.at[cp, s, n],
                      rh.at[cp, 2, s * 2 + n], dp, mp_of(g, mod4(a + SIGN[s])))

    def w_x(cp, s, j):
        ref = xb.at[cp, mod4(g - SIGN[s]), j]
        remote(ref, ref, sx.at[0, s, j], rx.at[cp, s, j], dp, mp).wait_recv()

    def w_xf(cp, s):
        ref = xb.at[cp, mod4(g + 2), s]
        remote(ref, ref, sxf.at[0, s], rx.at[cp, 2, s], dp, mp).wait_recv()

    def w_relay(cp, s, n):
        ref = rb.at[cp, s, n]
        remote(ref, ref, sr.at[0, s, n], rr.at[cp, s, n], dp, mp).wait_recv()

    def w_h(cp, s, n):
        ref = hb.at[cp, mod4(g + OFF[n]), :, mod4(a - SIGN[s])]
        remote(ref, ref, sh.at[0, s, n], rh.at[cp, s, n], dp, mp).wait_recv()

    def w_hf(cp, s, n):
        ref = hb.at[cp, mod4(g + HALF[s][n]), :, mod4(a + 2)]
        remote(ref, ref, srf.at[0, s, n], rh.at[cp, 2, s * 2 + n], dp, mp).wait_recv()

    d_len_local.start()
    d_len.start()
    for k in range(2):
        @pl.when(c == k)
        def _():
            for d in d_own_local(k):
                d.start()

        @pl.when(c != k)
        def _():
            for d in d_own_remote(k):
                d.start()
    for q in range(2):
        for k in range(2):
            for s in range(2):
                d_x(k, s, q if s == 0 else 1 - q).start()
    for n in range(2):
        for k in range(2):
            for s in range(2):
                d_relay(k, s, n).start()

    f_row = lax.broadcasted_iota(jnp.int32, (256, 2 * ROWS), 0)
    column = lax.broadcasted_iota(jnp.int32, (256, 2 * ROWS), 1)
    for k in range(2):
        eb[k] = jnp.where(column == 2 * f_row + k, 1.0, 0.0).astype(BF16)
    npart[...] = jnp.zeros_like(npart)
    gpad[...] = jnp.zeros_like(gpad)

    d_len_local.wait()
    d_len.wait_recv()
    e_row = lax.broadcasted_iota(jnp.int32, (16, 32), 0)
    e_lane = lax.broadcasted_iota(jnp.int32, (16, 32), 1)
    e_place, e_half = lax.rem(lax.div(e_row, 2), 4), lax.rem(e_row, 2)
    wanted = mp_of(e_place, a) * 2 + e_half
    lens = jnp.where(e_row < 8, lb[0], lb[1]).astype(F32)
    len_col = jnp.sum(jnp.where(e_lane == wanted, lens, 0.0), axis=1, keepdims=True)
    slot = lax.broadcasted_iota(jnp.int32, (16, SLOT), 1).astype(F32)
    mask = jnp.where(slot < len_col, 1.0, 0.0)
    for e in range(16):
        mt[e] = mask[e : e + 1]

    def tiles(cp, i, m):
        for j in range(2):
            e = cp * 8 + i * 2 + j
            h = hb[cp, i, j, m] * mt[e].astype(BF16)
            p = jnp.dot(h, xb[cp, i, j], preferred_element_type=F32)
            p = jnp.sum((p * p).reshape(ROWS // 8, 8, D), axis=0)
            part = p[:, :128]
            for n in range(1, D // 128):
                part = part + p[:, n * 128 : (n + 1) * 128]
            npart[e] += part

    def loop(count, body):
        lax.fori_loop(0, count, lambda n, carry: (body(n), carry)[1], 0)

    for k in range(2):
        @pl.when(c == k)
        def _():
            for d in d_own_local(k):
                d.wait()
    own_x, own_h = xb.at[other, g], hb.at[other, :, :, a]
    remote(own_x, own_x, sxo, rxo, dp, mp).wait_recv()
    remote(own_h, own_h, sho, rho, dp, mp).wait_recv()

    for cp in range(2):
        for s in range(2):
            w_x(cp, s, s)
            d_xf(cp, s).start()
    for n in range(4):
        for k in range(2):
            for s in range(2):
                d_h(k, s, n).start()
    loop(2, lambda cp: tiles(cp, g, a))
    for cp in range(2):
        for s in range(2):
            w_x(cp, s, 1 - s)
    loop(4, lambda n: tiles(lax.div(n, 2), mod4(g + 1 + 2 * lax.rem(n, 2)), a))
    for n in range(2):
        for cp in range(2):
            for s in range(2):
                w_relay(cp, s, n)
                d_rf(cp, s, n).start()

    for n in range(3):
        for s in range(2):
            w_h(c, s, n)
        loop(2, lambda s: tiles(c, mod4(g + OFF[n]), mod4(a - 1 + 2 * s)))
    for cp in range(2):
        for s in range(2):
            w_xf(cp, s)
    loop(2, lambda cp: tiles(cp, mod4(g + 2), a))
    for s in range(2):
        w_h(c, s, 3)
    loop(2, lambda s: tiles(c, mod4(g + 2), mod4(a - 1 + 2 * s)))
    for n in range(4):
        for s in range(2):
            w_h(other, s, n)
        loop(2, lambda s: tiles(other, mod4(g + OFF[n]), mod4(a - 1 + 2 * s)))
        t, cp = n // 2, n % 2
        for s in range(2):
            w_hf(cp, s, t)
        loop(2, lambda s: tiles(cp, mod4(g + HALF[0][t] * (1 - s) + HALF[1][t] * s), mod4(a + 2)))

    spot = c * 16 + mp
    per_example = jnp.sum(npart[...], axis=1)
    col = jnp.sum(per_example, axis=1, keepdims=True)
    r16 = lax.broadcasted_iota(jnp.int32, (16, 128), 0)
    l16 = lax.broadcasted_iota(jnp.int32, (16, 128), 1)
    nb[spot] = jnp.sum(jnp.where(l16 == r16, col, 0.0), axis=0, keepdims=True)

    def d_norm(n):
        to = lax.rem(spot + n + 1, 32)
        return remote(nb.at[spot], nb.at[spot], sn.at[n], rn.at[spot],
                      y * 2 + lax.div(to, 16), lax.rem(to, 16))

    loop(31, lambda n: d_norm(n).start())

    def norm_wait(n):
        src = lax.rem(spot + n + 1, 32)
        remote(nb.at[src], nb.at[src], sn.at[n], rn.at[src], dp, mp).wait_recv()

    loop(31, norm_wait)
    rows = nb[...].reshape(32, 128)
    s0 = rows[0:4] + rows[4:8] + rows[8:12] + rows[12:16]
    s1 = jnp.concatenate(
        [jnp.sum(rows[16 + 4 * n : 20 + 4 * n], axis=0, keepdims=True) for n in range(4)], axis=0
    )

    def picked(table, index, shape):
        out = jnp.zeros(shape, F32)
        for n in range(4):
            out = out + jnp.where(index == n, table[n : n + 1], 0.0)
        return out

    def factor(squares):
        return clip_limit / jnp.maximum(jnp.sqrt(squares), clip_limit)

    mine = jnp.where(c == 0, s0, s1)
    others = jnp.where(c == 0, s1, s0)
    place16, half16 = lax.rem(lax.div(r16, 2), 4), lax.rem(r16, 2)
    squares = jnp.sum(
        jnp.where(l16 == r16, picked(mine, a, (16, 128)), 0.0)
        + jnp.where(l16 == lax.div(r16, 8) * 8 + a * 2 + half16, picked(others, place16, (16, 128)), 0.0),
        axis=1, keepdims=True,
    )
    scaled_mask = mask * factor(squares)
    for e in range(16):
        ft[e] = scaled_mask[e : e + 1]

    def block(m):
        for cp in range(2):
            total = None
            for i in range(4):
                for j in range(2):
                    h = (hb[cp, i, j, m].astype(F32) * ft[cp * 8 + i * 2 + j]).astype(BF16)
                    p = jnp.dot(h, xb[cp, i, j], preferred_element_type=F32)
                    total = p if total is None else total + p
            if cp == 0:
                gacc[...] = total
            else:
                gacc[...] += total

    def far(n):
        return 2 - n + 3 * (n // 2)

    def d_part(n):
        return remote(gs.at[n], gr.at[n], sg.at[n], rg.at[n], dp, mp_of(g, mod4(a + far(n))))

    def send_block(n):
        block(mod4(a + far(n)))
        gs[n] = gacc[...].astype(BF16)
        d_part(n).start()

    loop(3, send_block)
    block(a)

    r32 = lax.broadcasted_iota(jnp.int32, (32, 128), 0)
    l32 = lax.broadcasted_iota(jnp.int32, (32, 128), 1)
    x32, z32, j32 = lax.div(r32, 8), lax.rem(lax.div(r32, 2), 4), lax.rem(r32, 2)
    squares = jnp.sum(
        jnp.where(l32 == c * 8 + x32 * 2 + j32, picked(s0, z32, (32, 128)), 0.0)
        + jnp.where(l32 == c * 8 + z32 * 2 + j32, picked(s1, x32, (32, 128)), 0.0),
        axis=1, keepdims=True,
    )
    clip_ref[...] = jnp.sum(
        jnp.where(l32[:, :32] == r32[:, :32], factor(squares), 0.0), axis=0, keepdims=True
    )

    for n in range(3):
        remote(gr.at[n], gr.at[n], sg.at[n], rg.at[n], dp, mp).wait_recv()
    gpad[0:ROWS] = gacc[...] + gr[0].astype(F32) + gr[1].astype(F32) + gr[2].astype(F32)
    turned = gpad[...].T.astype(BF16)
    for b in range(8):
        ys[b] = turned[b * OWN : (b + 1) * OWN]

    def d_y(dy, k):
        to_y = mod4(y + dy)
        return remote(ys.at[to_y * 2 + k], yr.at[c, dy], sy.at[dy, k], ry.at[c, dy], to_y * 2 + k, mp)

    for dy in (2, 1, 3):
        for k in range(2):
            d_y(dy, k).start()
    d_partner = remote(ys.at[y * 2 + other], yr.at[c, 0], sy.at[0, 0], ry.at[c, 0], y * 2 + other, mp)
    d_partner.start()
    total = jnp.dot(ys[dp], eb[c], preferred_element_type=F32)
    remote(yr.at[other, 0], yr.at[other, 0], sy.at[0, 1], ry.at[other, 0], dp, mp).wait_recv()
    total = total + jnp.dot(yr[other, 0], eb[other], preferred_element_type=F32)
    for dy in (1, 3, 2):
        for k in range(2):
            remote(yr.at[k, dy], yr.at[k, dy], sy.at[dy, k], ry.at[k, dy], dp, mp).wait_recv()
            total = total + jnp.dot(yr[k, dy], eb[k], preferred_element_type=F32)
    grad_ref[...] = total * (1.0 / EXAMPLES)

    d_len.wait_send()
    for k in range(2):
        @pl.when(c != k)
        def _():
            for d in d_own_remote(k):
                d.wait_send()
        for s in range(2):
            for j in range(2):
                d_x(k, s, j).wait_send()
                d_relay(k, s, j).wait_send()
                d_rf(k, s, j).wait_send()
            for n in range(4):
                d_h(k, s, n).wait_send()
            d_xf(k, s).wait_send()
    loop(31, lambda n: d_norm(n).wait_send())
    for n in range(3):
        d_part(n).wait_send()
    for dy in (2, 1, 3):
        for k in range(2):
            d_y(dy, k).wait_send()
    d_partner.wait_send()


def exchange(layer_input, output_cot, hidden_cot, hidden_act, lengths):
    dma = pltpu.SemaphoreType.DMA
    hbm = pl.BlockSpec(memory_space=pltpu.HBM)
    vmem = pl.BlockSpec(memory_space=pltpu.VMEM)
    return pl.pallas_call(
        kernel,
        out_shape=(jax.ShapeDtypeStruct((OWN, 2 * ROWS), F32), jax.ShapeDtypeStruct((1, 32), F32)),
        in_specs=[hbm] * 5,
        out_specs=(vmem, vmem),
        scratch_shapes=[
            pltpu.VMEM((2, 4, 2, SLOT, D), BF16),
            pltpu.VMEM((2, 4, 2, 4, ROWS, SLOT), BF16),
            pltpu.VMEM((2, 2, 2, 2, ROWS, SLOT), BF16),
            pltpu.VMEM((ROWS, D), F32),
            pltpu.VMEM((3, ROWS, D), BF16),
            pltpu.VMEM((3, ROWS, D), BF16),
            pltpu.VMEM((256, D), F32),
            pltpu.VMEM((8, OWN, 256), BF16),
            pltpu.VMEM((2, 4, OWN, 256), BF16),
            pltpu.VMEM((2, 256, 2 * ROWS), BF16),
            pltpu.VMEM((2, 1, 32), jnp.int32),
            pltpu.VMEM((16, 1, SLOT), F32),
            pltpu.VMEM((16, 1, SLOT), F32),
            pltpu.VMEM((16, 8, 128), F32),
            pltpu.VMEM((32, 1, 128), F32),
            dma((2,)), dma, dma((2, 2, 2)), dma, dma((2, 2, 2)), dma((2, 2, 4)), dma, dma, dma((2, 2)),
            dma((2, 2, 2)), dma((31,)), dma((3,)), dma((4, 2)),
            dma((2, 3, 2)), dma, dma((2, 2, 2)), dma((2, 3, 4)), dma, dma, dma((32,)), dma((3,)), dma((2, 4)),
        ],
        compiler_params=pltpu.CompilerParams(has_side_effects=True, vmem_limit_bytes=60 * 1024 * 1024),
    )(layer_input, output_cot, hidden_cot, hidden_act, lengths)


def local(
    layer_input, output_cot, hidden_act, hidden_cot, lengths, weights, moment_one, moment_two
):
    by_place = (4, 4, 2, ROWS, SLOT)
    gradient, clip = exchange(
        layer_input, output_cot, hidden_cot.reshape(by_place), hidden_act.reshape(by_place), lengths.reshape(1, 32)
    )
    new_moment_one = beta_one * moment_one + (1.0 - beta_one) * gradient
    new_moment_two = beta_two * moment_two + (1.0 - beta_two) * gradient * gradient
    corr_one = 1.0 - beta_one**STEP
    corr_two = 1.0 - beta_two**STEP
    direction = new_moment_one / corr_one / (jnp.sqrt(new_moment_two / corr_two) + adam_eps)
    new_weights = weights - learn_rate * (direction + weight_decay * weights)
    return (new_weights, new_moment_one, new_moment_two, clip.reshape(32))


def solution(mesh):
    return jax.shard_map(
        local,
        mesh=mesh,
        in_specs=(
            P(("dp", "mp"), None, None),
            P(("dp", "mp"), None, None),
            P("dp", "mp", None),
            P("dp", "mp", None),
            P("dp"),
            P("dp", "mp"),
            P("dp", "mp"),
            P("dp", "mp"),
        ),
        out_specs=(P("dp", "mp"), P("dp", "mp"), P("dp", "mp"), P("dp")),
        check_vma=False,
    )
```

```python
import math

import jax
import jax.numpy as jnp
from jax import lax
from jax.experimental import pallas as pl
from jax.experimental.pallas import tpu as pltpu
from jax.sharding import PartitionSpec as P

D = 768
FF = 3072
SLOT = 256
STEP = 10
EXAMPLES = 256
ROWS = 192
OWN = 96

beta_one = 0.9
beta_two = 0.999
adam_eps = 1e-08
learn_rate = 0.001
weight_decay = 0.01
clip_limit = 0.5 * math.sqrt(2.0 * D * FF * SLOT)

MESH = pl.DeviceIdType.MESH
BF16 = jnp.bfloat16
F32 = jnp.float32


def kernel(
    x0_ref, x1_ref, h0_ref, h1_ref, len_ref,
    grad_ref, clip_ref,
    xb, hb, rb, gacc, gs, gr, gpad, ys, yr, eb, lb, mt, ft, npart, nb,
    lsem, llen, sx, sxo, sr, sh, sho, slen, sxf, srf, sn, sg, sy,
    rx, rxo, rr, rh, rho, rlen, rn, rg, ry, near,
):
    dp, mp = lax.axis_index("dp"), lax.axis_index("mp")
    c, y = lax.rem(dp, 2), lax.div(dp, 2)
    x, z = lax.div(mp, 4), lax.rem(mp, 4)
    other = 1 - c
    mod4 = lambda v: lax.rem(v + 8, 4)
    g = c * z + (1 - c) * x
    a = c * x + (1 - c) * z
    mp_of = lambda gg, aa: (1 - c) * (gg * 4 + aa) + c * (aa * 4 + gg)

    def remote(src, dst, ssem, rsem, to_dp, to_mp):
        return pltpu.make_async_remote_copy(
            src_ref=src, dst_ref=dst, send_sem=ssem, recv_sem=rsem,
            device_id={"dp": to_dp, "mp": to_mp}, device_id_type=MESH,
        )

    x_refs, h_refs = (x0_ref, x1_ref), (h0_ref, h1_ref)
    SIGN = (1, -1)
    OFF = (0, 1, 3, 2)
    HALF = ((0, 1), (3, 2))

    def place(k):
        return (x, z) if k == 0 else (z, x)

    def mp_k(k, gg, aa):
        return gg * 4 + aa if k == 0 else aa * 4 + gg

    def h_slice(k, i, aa):
        return h_refs[k].at[i, aa] if k == 0 else h_refs[k].at[aa, i]

    def h_all(k, aa):
        return h_refs[k].at[:, aa] if k == 0 else h_refs[k].at[aa]

    def d_x(k, s, j):
        gk, ak = place(k)
        return remote(x_refs[k].at[j], xb.at[c, gk, j], sx.at[k, s, j], rx.at[c, s, j],
                      y * 2 + k, mp_k(k, mod4(gk + SIGN[s]), ak))

    def d_relay(k, s, n):
        gk, ak = place(k)
        i = mod4(gk + HALF[s][n])
        return remote(h_slice(k, i, mod4(ak + 2)), rb.at[c, s, n], sr.at[k, s, n], rr.at[c, s, n],
                      y * 2 + k, mp_k(k, gk, mod4(ak + SIGN[s])))

    def d_h(k, s, n):
        gk, ak = place(k)
        i = mod4(gk + OFF[n])
        aa = mod4(ak + SIGN[s])
        return remote(h_slice(k, i, aa), hb.at[c, i, :, ak], sh.at[k, s, n], rh.at[c, s, n],
                      y * 2 + k, mp_k(k, gk, aa))

    def d_own_remote(k):
        gk, ak = place(k)
        return (
            remote(x_refs[k], xb.at[c, gk], sxo, rxo, y * 2 + k, mp),
            remote(h_all(k, ak), hb.at[c, :, :, ak], sho, rho, y * 2 + k, mp),
        )

    def d_own_local(k):
        gk, ak = place(k)
        return (
            pltpu.make_async_copy(x_refs[k], xb.at[c, gk], lsem.at[0]),
            pltpu.make_async_copy(h_all(k, ak), hb.at[c, :, :, ak], lsem.at[1]),
        )

    d_len = remote(len_ref, lb.at[c], slen, rlen, y * 2 + other, mp)
    d_len_local = pltpu.make_async_copy(len_ref, lb.at[c], llen)

    def d_xf(cp, s):
        src = xb.at[cp, mod4(g - SIGN[s]), s]
        return remote(src, src, sxf.at[cp, s], rx.at[cp, 2, s], dp, mp_of(mod4(g + SIGN[s]), a))

    def d_rf(cp, s, n):
        i = mod4(g + HALF[s][n])
        return remote(rb.at[cp, s, n], hb.at[cp, i, :, mod4(a - SIGN[s])], srf.at[cp, s, n],
                      rh.at[cp, 2, s * 2 + n], dp, mp_of(g, mod4(a + SIGN[s])))

    def w_x(cp, s, j):
        ref = xb.at[cp, mod4(g - SIGN[s]), j]
        remote(ref, ref, sx.at[0, s, j], rx.at[cp, s, j], dp, mp).wait_recv()

    def w_xf(cp, s):
        ref = xb.at[cp, mod4(g + 2), s]
        remote(ref, ref, sxf.at[0, s], rx.at[cp, 2, s], dp, mp).wait_recv()

    def w_relay(cp, s, n):
        ref = rb.at[cp, s, n]
        remote(ref, ref, sr.at[0, s, n], rr.at[cp, s, n], dp, mp).wait_recv()

    def w_h(cp, s, n):
        ref = hb.at[cp, mod4(g + OFF[n]), :, mod4(a - SIGN[s])]
        remote(ref, ref, sh.at[0, s, n], rh.at[cp, s, n], dp, mp).wait_recv()

    def w_hf(cp, s, n):
        ref = hb.at[cp, mod4(g + HALF[s][n]), :, mod4(a + 2)]
        remote(ref, ref, srf.at[0, s, n], rh.at[cp, 2, s * 2 + n], dp, mp).wait_recv()

    def signal(sem, to_dp, to_mp):
        pl.semaphore_signal(sem, inc=1, device_id={"dp": to_dp, "mp": to_mp}, device_id_type=MESH)

    in_x = [mod4(x + s) * 4 + z for s in SIGN]
    in_z = [x * 4 + mod4(z + s) for s in SIGN]
    in_y = [mod4(y + s) * 2 for s in SIGN]
    barrier = pltpu.get_barrier_semaphore()
    signal(barrier, y * 2 + other, mp)
    for k in range(2):
        for to_mp in in_x + in_z:
            signal(barrier, y * 2 + k, to_mp)
        for to_dp in in_y:
            signal(barrier, to_dp + k, mp)
    pl.semaphore_wait(barrier, 13)

    d_len_local.start()
    d_len.start()
    for k in range(2):
        @pl.when(c == k)
        def _():
            for d in d_own_local(k):
                d.start()

        @pl.when(c != k)
        def _():
            for d in d_own_remote(k):
                d.start()
    for q in range(2):
        for k in range(2):
            for s in range(2):
                d_x(k, s, q if s == 0 else 1 - q).start()
    for n in range(2):
        for k in range(2):
            for s in range(2):
                d_relay(k, s, n).start()

    for to_mp in in_x:
        signal(near.at[0], dp, to_mp)
    for to_dp in in_y:
        signal(near.at[0], to_dp + c, mp)

    f_row = lax.broadcasted_iota(jnp.int32, (256, 2 * ROWS), 0)
    column = lax.broadcasted_iota(jnp.int32, (256, 2 * ROWS), 1)
    for k in range(2):
        eb[k] = jnp.where(column == 2 * f_row + k, 1.0, 0.0).astype(BF16)
    npart[...] = jnp.zeros_like(npart)
    gpad[...] = jnp.zeros_like(gpad)

    d_len_local.wait()
    d_len.wait_recv()
    e_row = lax.broadcasted_iota(jnp.int32, (16, 32), 0)
    e_lane = lax.broadcasted_iota(jnp.int32, (16, 32), 1)
    e_place, e_half = lax.rem(lax.div(e_row, 2), 4), lax.rem(e_row, 2)
    wanted = mp_of(e_place, a) * 2 + e_half
    lens = jnp.where(e_row < 8, lb[0], lb[1]).astype(F32)
    len_col = jnp.sum(jnp.where(e_lane == wanted, lens, 0.0), axis=1, keepdims=True)
    slot = lax.broadcasted_iota(jnp.int32, (16, SLOT), 1).astype(F32)
    mask = jnp.where(slot < len_col, 1.0, 0.0)
    for e in range(16):
        mt[e] = mask[e : e + 1]

    def tiles(cp, i, m):
        for j in range(2):
            e = cp * 8 + i * 2 + j
            h = hb[cp, i, j, m] * mt[e].astype(BF16)
            p = jnp.dot(h, xb[cp, i, j], preferred_element_type=F32)
            p = jnp.sum((p * p).reshape(ROWS // 8, 8, D), axis=0)
            part = p[:, :128]
            for n in range(1, D // 128):
                part = part + p[:, n * 128 : (n + 1) * 128]
            npart[e] += part

    def loop(count, body):
        lax.fori_loop(0, count, lambda n, carry: (body(n), carry)[1], 0)

    for k in range(2):
        @pl.when(c == k)
        def _():
            for d in d_own_local(k):
                d.wait()
    own_x, own_h = xb.at[other, g], hb.at[other, :, :, a]
    remote(own_x, own_x, sxo, rxo, dp, mp).wait_recv()
    remote(own_h, own_h, sho, rho, dp, mp).wait_recv()

    for cp in range(2):
        for s in range(2):
            w_x(cp, s, s)
            d_xf(cp, s).start()
    for n in range(4):
        for k in range(2):
            for s in range(2):
                d_h(k, s, n).start()
    loop(2, lambda cp: tiles(cp, g, a))
    pl.semaphore_wait(near.at[0], 4)
    for to_mp in in_z:
        signal(near.at[1], dp, to_mp)
    for cp in range(2):
        for s in range(2):
            w_x(cp, s, 1 - s)
    loop(4, lambda n: tiles(lax.div(n, 2), mod4(g + 1 + 2 * lax.rem(n, 2)), a))
    for n in range(2):
        for cp in range(2):
            for s in range(2):
                w_relay(cp, s, n)
                d_rf(cp, s, n).start()

    pl.semaphore_wait(near.at[1], 2)
    for to_mp in in_z:
        signal(near.at[2], dp, to_mp)

    for n in range(3):
        for s in range(2):
            w_h(c, s, n)
        loop(2, lambda s: tiles(c, mod4(g + OFF[n]), mod4(a - 1 + 2 * s)))
    for cp in range(2):
        for s in range(2):
            w_xf(cp, s)
    loop(2, lambda cp: tiles(cp, mod4(g + 2), a))
    for s in range(2):
        w_h(c, s, 3)
    loop(2, lambda s: tiles(c, mod4(g + 2), mod4(a - 1 + 2 * s)))
    pl.semaphore_wait(near.at[2], 2)
    for n in range(4):
        for s in range(2):
            w_h(other, s, n)
        loop(2, lambda s: tiles(other, mod4(g + OFF[n]), mod4(a - 1 + 2 * s)))
        t, cp = n // 2, n % 2
        for s in range(2):
            w_hf(cp, s, t)
        loop(2, lambda s: tiles(cp, mod4(g + HALF[0][t] * (1 - s) + HALF[1][t] * s), mod4(a + 2)))

    spot = c * 16 + mp
    per_example = jnp.sum(npart[...], axis=1)
    col = jnp.sum(per_example, axis=1, keepdims=True)
    r16 = lax.broadcasted_iota(jnp.int32, (16, 128), 0)
    l16 = lax.broadcasted_iota(jnp.int32, (16, 128), 1)
    nb[spot] = jnp.sum(jnp.where(l16 == r16, col, 0.0), axis=0, keepdims=True)

    def d_norm(n):
        to = lax.rem(spot + n + 1, 32)
        return remote(nb.at[spot], nb.at[spot], sn.at[n], rn.at[spot],
                      y * 2 + lax.div(to, 16), lax.rem(to, 16))

    loop(31, lambda n: d_norm(n).start())

    def norm_wait(n):
        src = lax.rem(spot + n + 1, 32)
        remote(nb.at[src], nb.at[src], sn.at[n], rn.at[src], dp, mp).wait_recv()

    loop(31, norm_wait)
    rows = nb[...].reshape(32, 128)
    s0 = rows[0:4] + rows[4:8] + rows[8:12] + rows[12:16]
    s1 = jnp.concatenate(
        [jnp.sum(rows[16 + 4 * n : 20 + 4 * n], axis=0, keepdims=True) for n in range(4)], axis=0
    )

    def picked(table, index, shape):
        out = jnp.zeros(shape, F32)
        for n in range(4):
            out = out + jnp.where(index == n, table[n : n + 1], 0.0)
        return out

    def factor(squares):
        return clip_limit / jnp.maximum(jnp.sqrt(squares), clip_limit)

    mine = jnp.where(c == 0, s0, s1)
    others = jnp.where(c == 0, s1, s0)
    place16, half16 = lax.rem(lax.div(r16, 2), 4), lax.rem(r16, 2)
    squares = jnp.sum(
        jnp.where(l16 == r16, picked(mine, a, (16, 128)), 0.0)
        + jnp.where(l16 == lax.div(r16, 8) * 8 + a * 2 + half16, picked(others, place16, (16, 128)), 0.0),
        axis=1, keepdims=True,
    )
    scaled_mask = mask * factor(squares)
    for e in range(16):
        ft[e] = scaled_mask[e : e + 1]

    def block(m):
        for cp in range(2):
            total = None
            for i in range(4):
                for j in range(2):
                    h = (hb[cp, i, j, m].astype(F32) * ft[cp * 8 + i * 2 + j]).astype(BF16)
                    p = jnp.dot(h, xb[cp, i, j], preferred_element_type=F32)
                    total = p if total is None else total + p
            if cp == 0:
                gacc[...] = total
            else:
                gacc[...] += total

    def far(n):
        return 2 - n + 3 * (n // 2)

    def d_part(n):
        return remote(gs.at[n], gr.at[n], sg.at[n], rg.at[n], dp, mp_of(g, mod4(a + far(n))))

    def send_block(n):
        block(mod4(a + far(n)))
        gs[n] = gacc[...].astype(BF16)
        d_part(n).start()

    loop(3, send_block)
    block(a)

    r32 = lax.broadcasted_iota(jnp.int32, (32, 128), 0)
    l32 = lax.broadcasted_iota(jnp.int32, (32, 128), 1)
    x32, z32, j32 = lax.div(r32, 8), lax.rem(lax.div(r32, 2), 4), lax.rem(r32, 2)
    squares = jnp.sum(
        jnp.where(l32 == c * 8 + x32 * 2 + j32, picked(s0, z32, (32, 128)), 0.0)
        + jnp.where(l32 == c * 8 + z32 * 2 + j32, picked(s1, x32, (32, 128)), 0.0),
        axis=1, keepdims=True,
    )
    clip_ref[...] = jnp.sum(
        jnp.where(l32[:, :32] == r32[:, :32], factor(squares), 0.0), axis=0, keepdims=True
    )

    for n in range(3):
        remote(gr.at[n], gr.at[n], sg.at[n], rg.at[n], dp, mp).wait_recv()
    gpad[0:ROWS] = gacc[...] + gr[0].astype(F32) + gr[1].astype(F32) + gr[2].astype(F32)
    turned = gpad[...].T.astype(BF16)
    for b in range(8):
        ys[b] = turned[b * OWN : (b + 1) * OWN]

    def d_y(dy, k):
        to_y = mod4(y + dy)
        return remote(ys.at[to_y * 2 + k], yr.at[c, dy], sy.at[dy, k], ry.at[c, dy], to_y * 2 + k, mp)

    for dy in (2, 1, 3):
        for k in range(2):
            d_y(dy, k).start()
    d_partner = remote(ys.at[y * 2 + other], yr.at[c, 0], sy.at[0, 0], ry.at[c, 0], y * 2 + other, mp)
    d_partner.start()
    total = jnp.dot(ys[dp], eb[c], preferred_element_type=F32)
    remote(yr.at[other, 0], yr.at[other, 0], sy.at[0, 1], ry.at[other, 0], dp, mp).wait_recv()
    total = total + jnp.dot(yr[other, 0], eb[other], preferred_element_type=F32)
    for dy in (1, 3, 2):
        for k in range(2):
            remote(yr.at[k, dy], yr.at[k, dy], sy.at[dy, k], ry.at[k, dy], dp, mp).wait_recv()
            total = total + jnp.dot(yr[k, dy], eb[k], preferred_element_type=F32)
    grad_ref[...] = total * (1.0 / EXAMPLES)

    d_len.wait_send()
    for k in range(2):
        @pl.when(c != k)
        def _():
            for d in d_own_remote(k):
                d.wait_send()
        for s in range(2):
            for j in range(2):
                d_x(k, s, j).wait_send()
                d_relay(k, s, j).wait_send()
                d_rf(k, s, j).wait_send()
            for n in range(4):
                d_h(k, s, n).wait_send()
            d_xf(k, s).wait_send()
    loop(31, lambda n: d_norm(n).wait_send())
    for n in range(3):
        d_part(n).wait_send()
    for dy in (2, 1, 3):
        for k in range(2):
            d_y(dy, k).wait_send()
    d_partner.wait_send()


def exchange(layer_input, output_cot, hidden_cot, hidden_act, lengths):
    dma = pltpu.SemaphoreType.DMA
    hbm = pl.BlockSpec(memory_space=pltpu.HBM)
    vmem = pl.BlockSpec(memory_space=pltpu.VMEM)
    return pl.pallas_call(
        kernel,
        out_shape=(jax.ShapeDtypeStruct((OWN, 2 * ROWS), F32), jax.ShapeDtypeStruct((1, 32), F32)),
        in_specs=[hbm] * 5,
        out_specs=(vmem, vmem),
        scratch_shapes=[
            pltpu.VMEM((2, 4, 2, SLOT, D), BF16),
            pltpu.VMEM((2, 4, 2, 4, ROWS, SLOT), BF16),
            pltpu.VMEM((2, 2, 2, 2, ROWS, SLOT), BF16),
            pltpu.VMEM((ROWS, D), F32),
            pltpu.VMEM((3, ROWS, D), BF16),
            pltpu.VMEM((3, ROWS, D), BF16),
            pltpu.VMEM((256, D), F32),
            pltpu.VMEM((8, OWN, 256), BF16),
            pltpu.VMEM((2, 4, OWN, 256), BF16),
            pltpu.VMEM((2, 256, 2 * ROWS), BF16),
            pltpu.VMEM((2, 1, 32), jnp.int32),
            pltpu.VMEM((16, 1, SLOT), F32),
            pltpu.VMEM((16, 1, SLOT), F32),
            pltpu.VMEM((16, 8, 128), F32),
            pltpu.VMEM((32, 1, 128), F32),
            dma((2,)), dma, dma((2, 2, 2)), dma, dma((2, 2, 2)), dma((2, 2, 4)), dma, dma, dma((2, 2)),
            dma((2, 2, 2)), dma((31,)), dma((3,)), dma((4, 2)),
            dma((2, 3, 2)), dma, dma((2, 2, 2)), dma((2, 3, 4)), dma, dma, dma((32,)), dma((3,)), dma((2, 4)),
            pltpu.SemaphoreType.REGULAR((3,)),
        ],
        compiler_params=pltpu.CompilerParams(has_side_effects=True, collective_id=0, vmem_limit_bytes=60 * 1024 * 1024),
    )(layer_input, output_cot, hidden_cot, hidden_act, lengths)


def local(
    layer_input, output_cot, hidden_act, hidden_cot, lengths, weights, moment_one, moment_two
):
    by_place = (4, 4, 2, ROWS, SLOT)
    gradient, clip = exchange(
        layer_input, output_cot, hidden_cot.reshape(by_place), hidden_act.reshape(by_place), lengths.reshape(1, 32)
    )
    new_moment_one = beta_one * moment_one + (1.0 - beta_one) * gradient
    new_moment_two = beta_two * moment_two + (1.0 - beta_two) * gradient * gradient
    corr_one = 1.0 - beta_one**STEP
    corr_two = 1.0 - beta_two**STEP
    direction = new_moment_one / corr_one / (jnp.sqrt(new_moment_two / corr_two) + adam_eps)
    new_weights = weights - learn_rate * (direction + weight_decay * weights)
    return (new_weights, new_moment_one, new_moment_two, clip.reshape(32))


def solution(mesh):
    return jax.shard_map(
        local,
        mesh=mesh,
        in_specs=(
            P(("dp", "mp"), None, None),
            P(("dp", "mp"), None, None),
            P("dp", "mp", None),
            P("dp", "mp", None),
            P("dp"),
            P("dp", "mp"),
            P("dp", "mp"),
            P("dp", "mp"),
        ),
        out_specs=(P("dp", "mp"), P("dp", "mp"), P("dp", "mp"), P("dp")),
        check_vma=False,
    )
```

```python
import math

import jax
import jax.numpy as jnp
from jax import lax
from jax.experimental import pallas as pl
from jax.experimental.pallas import tpu as pltpu
from jax.sharding import PartitionSpec as P

D = 768
FF = 3072
SLOT = 256
STEP = 10
EXAMPLES = 256
ROWS = 192
OWN = 96

beta_one = 0.9
beta_two = 0.999
adam_eps = 1e-08
learn_rate = 0.001
weight_decay = 0.01
clip_limit = 0.5 * math.sqrt(2.0 * D * FF * SLOT)

MESH = pl.DeviceIdType.MESH
BF16 = jnp.bfloat16
F32 = jnp.float32


def kernel(
    x0_ref, x1_ref, h0_ref, h1_ref, len_ref,
    grad_ref, clip_ref,
    xb, hb, gall, gs, gr, gpad, ys, yr, eb, lb, mt, ft, npart, nb,
    lsem, llen, sx, sxo, sh, sho, slen, sxf, sn, sg, sy,
    rx, rxo, rh, rho, rlen, rn, rg, ry, near,
):
    dp, mp = lax.axis_index("dp"), lax.axis_index("mp")
    c, y = lax.rem(dp, 2), lax.div(dp, 2)
    x, z = lax.div(mp, 4), lax.rem(mp, 4)
    other = 1 - c
    mod4 = lambda v: lax.rem(v + 8, 4)
    g = c * z + (1 - c) * x
    a = c * x + (1 - c) * z
    mp_of = lambda gg, aa: (1 - c) * (gg * 4 + aa) + c * (aa * 4 + gg)

    def remote(src, dst, ssem, rsem, to_dp, to_mp):
        return pltpu.make_async_remote_copy(
            src_ref=src, dst_ref=dst, send_sem=ssem, recv_sem=rsem,
            device_id={"dp": to_dp, "mp": to_mp}, device_id_type=MESH,
        )

    def signal(sem, to_dp, to_mp):
        pl.semaphore_signal(sem, inc=1, device_id={"dp": to_dp, "mp": to_mp}, device_id_type=MESH)

    def loop(count, body):
        lax.fori_loop(0, count, lambda n, carry: (body(n), carry)[1], 0)

    x_refs, h_refs = (x0_ref, x1_ref), (h0_ref, h1_ref)
    STEPS = (1, -1, 2)
    CHUNK = ROWS // 2

    def place(k):
        return (x, z) if k == 0 else (z, x)

    def mp_k(k, gg, aa):
        return gg * 4 + aa if k == 0 else aa * 4 + gg

    def h_slice(k, i, aa):
        return h_refs[k].at[i, aa] if k == 0 else h_refs[k].at[aa, i]

    def h_all(k, aa):
        return h_refs[k].at[:, aa] if k == 0 else h_refs[k].at[aa]

    def d_x(k, s, j):
        gk, ak = place(k)
        return remote(x_refs[k].at[j], xb.at[c, gk, j], sx.at[k, s, j], rx.at[c, s, j],
                      y * 2 + k, mp_k(k, mod4(gk + STEPS[s]), ak))

    def d_h(k, s, r):
        gk, ak = place(k)
        aa = mod4(ak + STEPS[s])
        i = mod4(r - aa)
        return remote(h_slice(k, i, aa), hb.at[c, i, :, ak], sh.at[k, s, r], rh.at[c, s, r],
                      y * 2 + k, mp_k(k, gk, aa))

    def d_own_remote(k):
        gk, ak = place(k)
        return (
            remote(x_refs[k], xb.at[c, gk], sxo, rxo, y * 2 + k, mp),
            remote(h_all(k, ak), hb.at[c, :, :, ak], sho, rho, y * 2 + k, mp),
        )

    def d_own_local(k):
        gk, ak = place(k)
        return (
            pltpu.make_async_copy(x_refs[k], xb.at[c, gk], lsem.at[0]),
            pltpu.make_async_copy(h_all(k, ak), hb.at[c, :, :, ak], lsem.at[1]),
        )

    d_len = remote(len_ref, lb.at[c], slen, rlen, y * 2 + other, mp)
    d_len_local = pltpu.make_async_copy(len_ref, lb.at[c], llen)

    def d_xf(cp, s):
        src = xb.at[cp, mod4(g - STEPS[s]), s]
        return remote(src, src, sxf.at[cp, s], rx.at[cp, 2, s], dp, mp_of(mod4(g + STEPS[s]), a))

    def w_x(cp, s, j):
        ref = xb.at[cp, mod4(g - STEPS[s]), j]
        remote(ref, ref, sx.at[0, s, j], rx.at[cp, s, j], dp, mp).wait_recv()

    def w_xf(cp, s):
        ref = xb.at[cp, mod4(g + 2), s]
        remote(ref, ref, sxf.at[0, s], rx.at[cp, 2, s], dp, mp).wait_recv()

    def w_h(cp, s, r):
        ref = hb.at[cp, mod4(r - a), :, mod4(a - STEPS[s])]
        remote(ref, ref, sh.at[0, s, r], rh.at[cp, s, r], dp, mp).wait_recv()

    in_x = [mod4(x + s) * 4 + z for s in STEPS[:2]]
    in_z = [x * 4 + mod4(z + s) for s in STEPS[:2]]
    in_y = [mod4(y + s) * 2 for s in STEPS[:2]]
    barrier = pltpu.get_barrier_semaphore()
    signal(barrier, y * 2 + other, mp)
    for k in range(2):
        for to_mp in in_x + in_z:
            signal(barrier, y * 2 + k, to_mp)
        for to_dp in in_y:
            signal(barrier, to_dp + k, mp)
    pl.semaphore_wait(barrier, 13)

    for q in range(2):
        for k in range(2):
            for s in range(2):
                d_x(k, s, q if s == 0 else 1 - q).start()
    d_len_local.start()
    d_len.start()
    for k in range(2):
        @pl.when(c == k)
        def _():
            for d in d_own_local(k):
                d.start()

        @pl.when(c != k)
        def _():
            for d in d_own_remote(k):
                d.start()
    for to_mp in in_x + in_z:
        signal(near.at[0], dp, to_mp)
    for to_dp in in_y:
        signal(near.at[0], to_dp + c, mp)

    f_row = lax.broadcasted_iota(jnp.int32, (128, 2 * ROWS), 0)
    column = lax.broadcasted_iota(jnp.int32, (128, 2 * ROWS), 1)
    for k in range(2):
        for h in range(2):
            hit = jnp.where(column == 2 * (f_row + h * CHUNK) + k, 1.0, 0.0)
            eb[k, h] = jnp.where(f_row < CHUNK, hit, 0.0).astype(BF16)
    npart[...] = jnp.zeros_like(npart)
    gpad[...] = jnp.zeros_like(gpad)

    d_len_local.wait()
    d_len.wait_recv()
    e_row = lax.broadcasted_iota(jnp.int32, (16, 32), 0)
    e_lane = lax.broadcasted_iota(jnp.int32, (16, 32), 1)
    e_place, e_half = lax.rem(lax.div(e_row, 2), 4), lax.rem(e_row, 2)
    wanted = mp_of(e_place, a) * 2 + e_half
    lens = jnp.where(e_row < 8, lb[0], lb[1]).astype(F32)
    len_col = jnp.sum(jnp.where(e_lane == wanted, lens, 0.0), axis=1, keepdims=True)
    slot = lax.broadcasted_iota(jnp.int32, (16, SLOT), 1).astype(F32)
    mask = jnp.where(slot < len_col, 1.0, 0.0)
    for e in range(16):
        mt[e] = mask[e : e + 1]

    def tiles(cp, i, m):
        for j in range(2):
            e = cp * 8 + i * 2 + j
            h = hb[cp, i, j, m] * mt[e].astype(BF16)
            p = jnp.dot(h, xb[cp, i, j], preferred_element_type=F32)
            p = jnp.sum((p * p).reshape(ROWS // 8, 8, D), axis=0)
            part = p[:, :128]
            for n in range(1, D // 128):
                part = part + p[:, n * 128 : (n + 1) * 128]
            npart[e] += part

    for cp in range(2):
        for s in range(2):
            w_x(cp, s, s)
            d_xf(cp, s).start()
    pl.semaphore_wait(near.at[0], 6)
    for r in range(4):
        for s in (2, 0, 1):
            for k in range(2):
                d_h(k, s, r).start()
    for to_mp in in_z:
        signal(near.at[1], dp, to_mp)

    for k in range(2):
        @pl.when(c == k)
        def _():
            for d in d_own_local(k):
                d.wait()
    own_x, own_h = xb.at[other, g], hb.at[other, :, :, a]
    remote(own_x, own_x, sxo, rxo, dp, mp).wait_recv()
    remote(own_h, own_h, sho, rho, dp, mp).wait_recv()
    loop(2, lambda cp: tiles(cp, g, a))
    for cp in range(2):
        for s in range(2):
            w_x(cp, s, 1 - s)
    loop(4, lambda n: tiles(lax.div(n, 2), mod4(g + 1 + 2 * lax.rem(n, 2)), a))
    pl.semaphore_wait(near.at[1], 2)
    for to_mp in in_z:
        signal(near.at[2], dp, to_mp)
    for cp in range(2):
        for s in range(2):
            w_xf(cp, s)
    loop(2, lambda cp: tiles(cp, mod4(g + 2), a))
    pl.semaphore_wait(near.at[2], 2)

    spot = c * 16 + mp
    r16 = lax.broadcasted_iota(jnp.int32, (16, 128), 0)
    l16 = lax.broadcasted_iota(jnp.int32, (16, 128), 1)
    far_first = sorted(
        [(dx, dz, dk) for dx in range(4) for dz in range(4) for dk in range(2) if dx or dz or dk],
        key=lambda t: -(min(t[0], 4 - t[0]) + min(t[1], 4 - t[1])),
    )

    def norm_peer(n):
        dx, dz, dk = far_first[n]
        core = c if dk == 0 else other
        return core, mod4(x + dx) * 4 + mod4(z + dz)

    def d_norm(q, n):
        core, to_mp = norm_peer(n)
        return remote(nb.at[q, spot], nb.at[q, spot], sn.at[q, n], rn.at[q, spot], y * 2 + core, to_mp)

    def norm_send(q):
        col = jnp.sum(jnp.sum(npart[...], axis=1), axis=1, keepdims=True)
        nb[q, spot] = jnp.sum(jnp.where(l16 == r16, col, 0.0), axis=0, keepdims=True)
        for n in range(31):
            d_norm(q, n).start()

    def picked(table, index, shape):
        out = jnp.zeros(shape, F32)
        for n in range(4):
            out = out + jnp.where(index == n, table[n : n + 1], 0.0)
        return out

    def factor(squares):
        return clip_limit / jnp.maximum(jnp.sqrt(squares), clip_limit)

    def norm_take(q):
        for n in range(31):
            core, from_mp = norm_peer(n)
            ref = nb.at[q, core * 16 + from_mp]
            remote(ref, ref, sn.at[q, n], rn.at[q, core * 16 + from_mp], dp, mp).wait_recv()
        rows = nb[q].reshape(32, 128)
        s0 = rows[0:4] + rows[4:8] + rows[8:12] + rows[12:16]
        s1 = jnp.concatenate(
            [jnp.sum(rows[16 + 4 * n : 20 + 4 * n], axis=0, keepdims=True) for n in range(4)], axis=0
        )
        mine = jnp.where(c == 0, s0, s1)
        others = jnp.where(c == 0, s1, s0)
        place16, half16 = lax.rem(lax.div(r16, 2), 4), lax.rem(r16, 2)
        squares = jnp.sum(
            jnp.where(l16 == r16, picked(mine, a, (16, 128)), 0.0)
            + jnp.where(l16 == lax.div(r16, 8) * 8 + a * 2 + half16, picked(others, place16, (16, 128)), 0.0),
            axis=1, keepdims=True,
        )
        scaled_mask = mask * factor(squares)
        for e in range(16):
            ft[e] = scaled_mask[e : e + 1]
        return s0, s1

    for r in range(4):
        for s in (2, 0, 1):
            for cp in range(2):
                w_h(cp, s, r)
            loop(2, lambda cp: tiles(cp, mod4(r - a), mod4(a - STEPS[s])))
        if r >= 2:
            norm_send(r - 2)
    norm_take(0)

    def owner(n):
        return mod4(a + 2 - n + 3 * (n // 2) - 2 * (n // 3))

    def products(m, ranks):
        total = None
        for r in ranks:
            for cp in range(2):
                for j in range(2):
                    i = mod4(r - a)
                    h = (hb[cp, i, j, m].astype(F32) * ft[cp * 8 + i * 2 + j]).astype(BF16)
                    p = jnp.dot(h, xb[cp, i, j], preferred_element_type=F32)
                    total = p if total is None else total + p
        return total

    def early(n):
        gall[n] = products(owner(n), (0, 1, 2))

    loop(4, early)
    s0, s1 = norm_take(1)

    def d_part(n, h):
        rows = pl.ds(h * CHUNK, CHUNK)
        return remote(gs.at[n, rows], gr.at[n, rows], sg.at[n, h], rg.at[n, h], dp, mp_of(g, owner(n)))

    for n in range(4):
        total = gall[n] + products(owner(n), (3,))
        if n < 3:
            gs[n] = total.astype(BF16)
            d_part(n, 0).start()
        else:
            gall[n] = total
        if n == 2:
            for t in range(3):
                d_part(t, 1).start()

    r32 = lax.broadcasted_iota(jnp.int32, (32, 128), 0)
    l32 = lax.broadcasted_iota(jnp.int32, (32, 128), 1)
    x32, z32, j32 = lax.div(r32, 8), lax.rem(lax.div(r32, 2), 4), lax.rem(r32, 2)
    squares = jnp.sum(
        jnp.where(l32 == c * 8 + x32 * 2 + j32, picked(s0, z32, (32, 128)), 0.0)
        + jnp.where(l32 == c * 8 + z32 * 2 + j32, picked(s1, x32, (32, 128)), 0.0),
        axis=1, keepdims=True,
    )
    clip_ref[...] = jnp.sum(
        jnp.where(l32[:, :32] == r32[:, :32], factor(squares), 0.0), axis=0, keepdims=True
    )

    def d_y(h, dy, k):
        to_dp = mod4(y + dy) * 2 + k
        return remote(ys.at[h, to_dp], yr.at[h, c, dy], sy.at[h, dy, k], ry.at[h, c, dy], to_dp, mp)

    def d_partner(h):
        to_dp = y * 2 + other
        return remote(ys.at[h, to_dp], yr.at[h, c, 0], sy.at[h, 0, 0], ry.at[h, c, 0], to_dp, mp)

    for h in range(2):
        rows = pl.ds(h * CHUNK, CHUNK)
        for n in range(3):
            ref = gr.at[n, rows]
            remote(ref, ref, sg.at[n, h], rg.at[n, h], dp, mp).wait_recv()
        gpad[0:CHUNK] = (
            gall[3, rows] + gr[0, rows].astype(F32) + gr[1, rows].astype(F32) + gr[2, rows].astype(F32)
        )
        turned = gpad[...].T.astype(BF16)
        for b in range(8):
            ys[h, b] = turned[b * OWN : (b + 1) * OWN]
        for dy in (2, 1, 3):
            for k in range(2):
                d_y(h, dy, k).start()
        d_partner(h).start()
    total = jnp.dot(ys[0, dp], eb[c, 0], preferred_element_type=F32)
    total = total + jnp.dot(ys[1, dp], eb[c, 1], preferred_element_type=F32)
    for h in range(2):
        ref = yr.at[h, other, 0]
        remote(ref, ref, sy.at[h, 0, 1], ry.at[h, other, 0], dp, mp).wait_recv()
        total = total + jnp.dot(yr[h, other, 0], eb[other, h], preferred_element_type=F32)
        for dy in (1, 3, 2):
            for k in range(2):
                ref = yr.at[h, k, dy]
                remote(ref, ref, sy.at[h, dy, k], ry.at[h, k, dy], dp, mp).wait_recv()
                total = total + jnp.dot(yr[h, k, dy], eb[k, h], preferred_element_type=F32)
    grad_ref[...] = total * (1.0 / EXAMPLES)

    d_len.wait_send()
    for k in range(2):
        @pl.when(c != k)
        def _():
            for d in d_own_remote(k):
                d.wait_send()
        for s in range(2):
            for j in range(2):
                d_x(k, s, j).wait_send()
            d_xf(k, s).wait_send()
        for s in range(3):
            for r in range(4):
                d_h(k, s, r).wait_send()
    for q in range(2):
        for n in range(31):
            d_norm(q, n).wait_send()
    for h in range(2):
        for n in range(3):
            d_part(n, h).wait_send()
        for dy in (2, 1, 3):
            for k in range(2):
                d_y(h, dy, k).wait_send()
        d_partner(h).wait_send()


def exchange(layer_input, output_cot, hidden_cot, hidden_act, lengths):
    dma = pltpu.SemaphoreType.DMA
    hbm = pl.BlockSpec(memory_space=pltpu.HBM)
    vmem = pl.BlockSpec(memory_space=pltpu.VMEM)
    return pl.pallas_call(
        kernel,
        out_shape=(jax.ShapeDtypeStruct((OWN, 2 * ROWS), F32), jax.ShapeDtypeStruct((1, 32), F32)),
        in_specs=[hbm] * 5,
        out_specs=(vmem, vmem),
        scratch_shapes=[
            pltpu.VMEM((2, 4, 2, SLOT, D), BF16),
            pltpu.VMEM((2, 4, 2, 4, ROWS, SLOT), BF16),
            pltpu.VMEM((4, ROWS, D), F32),
            pltpu.VMEM((3, ROWS, D), BF16),
            pltpu.VMEM((3, ROWS, D), BF16),
            pltpu.VMEM((128, D), F32),
            pltpu.VMEM((2, 8, OWN, 128), BF16),
            pltpu.VMEM((2, 2, 4, OWN, 128), BF16),
            pltpu.VMEM((2, 2, 128, 2 * ROWS), BF16),
            pltpu.VMEM((2, 1, 32), jnp.int32),
            pltpu.VMEM((16, 1, SLOT), F32),
            pltpu.VMEM((16, 1, SLOT), F32),
            pltpu.VMEM((16, 8, 128), F32),
            pltpu.VMEM((2, 32, 1, 128), F32),
            dma((2,)), dma, dma((2, 2, 2)), dma, dma((2, 3, 4)), dma, dma, dma((2, 2)),
            dma((2, 31)), dma((3, 2)), dma((2, 4, 2)),
            dma((2, 3, 2)), dma, dma((2, 3, 4)), dma, dma, dma((2, 32)), dma((3, 2)), dma((2, 2, 4)),
            pltpu.SemaphoreType.REGULAR((3,)),
        ],
        compiler_params=pltpu.CompilerParams(has_side_effects=True, collective_id=0, vmem_limit_bytes=60 * 1024 * 1024),
    )(layer_input, output_cot, hidden_cot, hidden_act, lengths)


def adam_kernel(grad_ref, clip_ref, w_ref, m1_ref, m2_ref, new_w_ref, new_m1_ref, new_m2_ref, out_clip_ref):
    gradient, weights = grad_ref[...], w_ref[...]
    new_moment_one = beta_one * m1_ref[...] + (1.0 - beta_one) * gradient
    new_moment_two = beta_two * m2_ref[...] + (1.0 - beta_two) * gradient * gradient
    corr_one = 1.0 - beta_one**STEP
    corr_two = 1.0 - beta_two**STEP
    direction = new_moment_one / corr_one / (jnp.sqrt(new_moment_two / corr_two) + adam_eps)
    new_w_ref[...] = weights - learn_rate * (direction + weight_decay * weights)
    new_m1_ref[...] = new_moment_one
    new_m2_ref[...] = new_moment_two
    out_clip_ref[...] = clip_ref[...]


def local(
    layer_input, output_cot, hidden_act, hidden_cot, lengths, weights, moment_one, moment_two
):
    by_place = (4, 4, 2, ROWS, SLOT)
    gradient, clip = exchange(
        layer_input, output_cot, hidden_cot.reshape(by_place), hidden_act.reshape(by_place), lengths.reshape(1, 32)
    )
    state = jax.ShapeDtypeStruct((OWN, 2 * ROWS), F32)
    new_weights, new_moment_one, new_moment_two, clip_scale = pl.pallas_call(
        adam_kernel, out_shape=(state, state, state, jax.ShapeDtypeStruct((1, 32), F32))
    )(gradient, clip, weights, moment_one, moment_two)
    return (new_weights, new_moment_one, new_moment_two, clip_scale.reshape(32))


def solution(mesh):
    return jax.shard_map(
        local,
        mesh=mesh,
        in_specs=(
            P(("dp", "mp"), None, None),
            P(("dp", "mp"), None, None),
            P("dp", "mp", None),
            P("dp", "mp", None),
            P("dp"),
            P("dp", "mp"),
            P("dp", "mp"),
            P("dp", "mp"),
        ),
        out_specs=(P("dp", "mp"), P("dp", "mp"), P("dp", "mp"), P("dp")),
        check_vma=False,
    )
```

```python
import math

import jax
import jax.numpy as jnp
from jax import lax
from jax.experimental import pallas as pl
from jax.experimental.pallas import tpu as pltpu
from jax.sharding import PartitionSpec as P

D = 768
FF = 3072
SLOT = 256
STEP = 10
EXAMPLES = 256
ROWS = 192
OWN = 96

beta_one = 0.9
beta_two = 0.999
adam_eps = 1e-08
learn_rate = 0.001
weight_decay = 0.01
clip_limit = 0.5 * math.sqrt(2.0 * D * FF * SLOT)

MESH = pl.DeviceIdType.MESH
BF16 = jnp.bfloat16
F32 = jnp.float32


def kernel(
    x0_ref, x1_ref, h0_ref, h1_ref, len_ref,
    grad_ref, clip_ref,
    xb, hb, gall, gs, gr, gh, ys, yr, yhs, yhr, hs, hr, eb, eh, lb, mt, ft, npart, nb,
    lsem, llen, sx, sxo, sh, sho, slen, sxf, sn, sg, sy, syh, shh,
    rx, rxo, rh, rho, rlen, rn, rg, ry, ryh, rhh, near,
):
    dp, mp = lax.axis_index("dp"), lax.axis_index("mp")
    c, y = lax.rem(dp, 2), lax.div(dp, 2)
    x, z = lax.div(mp, 4), lax.rem(mp, 4)
    other = 1 - c
    mod4 = lambda v: lax.rem(v + 8, 4)
    g = c * z + (1 - c) * x
    a = c * x + (1 - c) * z
    mp_of = lambda gg, aa: (1 - c) * (gg * 4 + aa) + c * (aa * 4 + gg)

    def remote(src, dst, ssem, rsem, to_dp, to_mp):
        return pltpu.make_async_remote_copy(
            src_ref=src, dst_ref=dst, send_sem=ssem, recv_sem=rsem,
            device_id={"dp": to_dp, "mp": to_mp}, device_id_type=MESH,
        )

    def signal(sem, to_dp, to_mp):
        pl.semaphore_signal(sem, inc=1, device_id={"dp": to_dp, "mp": to_mp}, device_id_type=MESH)

    def loop(count, body):
        lax.fori_loop(0, count, lambda n, carry: (body(n), carry)[1], 0)

    x_refs, h_refs = (x0_ref, x1_ref), (h0_ref, h1_ref)
    STEPS = (1, -1, 2)
    LOW, HIGH = 128, ROWS - 128

    def place(k):
        return (x, z) if k == 0 else (z, x)

    def mp_k(k, gg, aa):
        return gg * 4 + aa if k == 0 else aa * 4 + gg

    def h_slice(k, i, aa):
        return h_refs[k].at[i, aa] if k == 0 else h_refs[k].at[aa, i]

    def h_all(k, aa):
        return h_refs[k].at[:, aa] if k == 0 else h_refs[k].at[aa]

    def d_x(k, s, j):
        gk, ak = place(k)
        return remote(x_refs[k].at[j], xb.at[c, gk, j], sx.at[k, s, j], rx.at[c, s, j],
                      y * 2 + k, mp_k(k, mod4(gk + STEPS[s]), ak))

    def d_h(k, s, q):
        gk, ak = place(k)
        aa = mod4(ak + STEPS[s])
        i = mod4(min(q, 3) - aa)
        src, dst = h_slice(k, i, aa), hb.at[c, i, :, ak]
        if q >= 3:
            src, dst = src.at[q - 3], hb.at[c, i, q - 3, ak]
        return remote(src, dst, sh.at[k, s, q], rh.at[c, s, q], y * 2 + k, mp_k(k, gk, aa))

    def d_own_remote(k):
        gk, ak = place(k)
        return (
            remote(x_refs[k], xb.at[c, gk], sxo, rxo, y * 2 + k, mp),
            remote(h_all(k, ak), hb.at[c, :, :, ak], sho, rho, y * 2 + k, mp),
        )

    def d_own_local(k):
        gk, ak = place(k)
        return (
            pltpu.make_async_copy(x_refs[k], xb.at[c, gk], lsem.at[0]),
            pltpu.make_async_copy(h_all(k, ak), hb.at[c, :, :, ak], lsem.at[1]),
        )

    d_len = remote(len_ref, lb.at[c], slen, rlen, y * 2 + other, mp)
    d_len_local = pltpu.make_async_copy(len_ref, lb.at[c], llen)

    def d_xf(cp, s):
        src = xb.at[cp, mod4(g - STEPS[s]), s]
        return remote(src, src, sxf.at[cp, s], rx.at[cp, 2, s], dp, mp_of(mod4(g + STEPS[s]), a))

    def w_x(cp, s, j):
        ref = xb.at[cp, mod4(g - STEPS[s]), j]
        remote(ref, ref, sx.at[0, s, j], rx.at[cp, s, j], dp, mp).wait_recv()

    def w_xf(cp, s):
        ref = xb.at[cp, mod4(g + 2), s]
        remote(ref, ref, sxf.at[0, s], rx.at[cp, 2, s], dp, mp).wait_recv()

    def w_h(cp, s, q):
        half = slice(None) if q < 3 else q - 3
        ref = hb.at[cp, mod4(min(q, 3) - a), half, mod4(a - STEPS[s])]
        remote(ref, ref, sh.at[0, s, q], rh.at[cp, s, q], dp, mp).wait_recv()

    in_x = [mod4(x + s) * 4 + z for s in STEPS[:2]]
    in_z = [x * 4 + mod4(z + s) for s in STEPS[:2]]
    in_y = [mod4(y + s) * 2 for s in STEPS[:2]]
    barrier = pltpu.get_barrier_semaphore()
    signal(barrier, y * 2 + other, mp)
    for k in range(2):
        for to_mp in in_x + in_z:
            signal(barrier, y * 2 + k, to_mp)
        for to_dp in in_y:
            signal(barrier, to_dp + k, mp)
    pl.semaphore_wait(barrier, 13)

    for q in range(2):
        for k in range(2):
            for s in range(2):
                d_x(k, s, q if s == 0 else 1 - q).start()
    d_len_local.start()
    d_len.start()
    for k in range(2):
        @pl.when(c == k)
        def _():
            for d in d_own_local(k):
                d.start()

        @pl.when(c != k)
        def _():
            for d in d_own_remote(k):
                d.start()
    for to_mp in in_x + in_z:
        signal(near.at[0], dp, to_mp)
    for to_dp in in_y:
        signal(near.at[0], to_dp + c, mp)

    f_row = lax.broadcasted_iota(jnp.int32, (128, 2 * ROWS), 0)
    column = lax.broadcasted_iota(jnp.int32, (128, 2 * ROWS), 1)
    for k in range(2):
        eb[k] = jnp.where(column == 2 * f_row + k, 1.0, 0.0).astype(BF16)
        high = f_row - HIGH * lax.rem(place(k)[1], 2)
        hit = jnp.where(column == 2 * (LOW + high) + k, 1.0, 0.0)
        eh[k] = jnp.where(high < HIGH, jnp.where(high >= 0, hit, 0.0), 0.0).astype(BF16)
    npart[...] = jnp.zeros_like(npart)

    d_len_local.wait()
    d_len.wait_recv()
    e_row = lax.broadcasted_iota(jnp.int32, (16, 32), 0)
    e_lane = lax.broadcasted_iota(jnp.int32, (16, 32), 1)
    e_place, e_half = lax.rem(lax.div(e_row, 2), 4), lax.rem(e_row, 2)
    wanted = mp_of(e_place, a) * 2 + e_half
    lens = jnp.where(e_row < 8, lb[0], lb[1]).astype(F32)
    len_col = jnp.sum(jnp.where(e_lane == wanted, lens, 0.0), axis=1, keepdims=True)
    slot = lax.broadcasted_iota(jnp.int32, (16, SLOT), 1).astype(F32)
    mask = jnp.where(slot < len_col, 1.0, 0.0)
    for e in range(16):
        mt[e] = mask[e : e + 1]

    def tiles(cp, i, m, halves=(0, 1)):
        for j in halves:
            e = cp * 8 + i * 2 + j
            h = hb[cp, i, j, m] * mt[e].astype(BF16)
            p = jnp.dot(h, xb[cp, i, j], preferred_element_type=F32)
            p = jnp.sum((p * p).reshape(ROWS // 8, 8, D), axis=0)
            part = p[:, :128]
            for n in range(1, D // 128):
                part = part + p[:, n * 128 : (n + 1) * 128]
            npart[e] += part

    for cp in range(2):
        for s in range(2):
            w_x(cp, s, s)
            d_xf(cp, s).start()
    pl.semaphore_wait(near.at[0], 6)
    for q in range(5):
        for s in (2, 0, 1):
            for k in range(2):
                d_h(k, s, q).start()
    for to_mp in in_z:
        signal(near.at[1], dp, to_mp)

    for k in range(2):
        @pl.when(c == k)
        def _():
            for d in d_own_local(k):
                d.wait()
    own_x, own_h = xb.at[other, g], hb.at[other, :, :, a]
    remote(own_x, own_x, sxo, rxo, dp, mp).wait_recv()
    remote(own_h, own_h, sho, rho, dp, mp).wait_recv()
    loop(2, lambda cp: tiles(cp, g, a))
    for cp in range(2):
        for s in range(2):
            w_x(cp, s, 1 - s)
    loop(4, lambda n: tiles(lax.div(n, 2), mod4(g + 1 + 2 * lax.rem(n, 2)), a))
    pl.semaphore_wait(near.at[1], 2)
    for to_mp in in_z:
        signal(near.at[2], dp, to_mp)
    for cp in range(2):
        for s in range(2):
            w_xf(cp, s)
    loop(2, lambda cp: tiles(cp, mod4(g + 2), a))
    pl.semaphore_wait(near.at[2], 2)

    spot = c * 16 + mp
    r16 = lax.broadcasted_iota(jnp.int32, (16, 128), 0)
    l16 = lax.broadcasted_iota(jnp.int32, (16, 128), 1)
    far_first = sorted(
        [(dx, dz, dk) for dx in range(4) for dz in range(4) for dk in range(2) if dx or dz or dk],
        key=lambda t: -(min(t[0], 4 - t[0]) + min(t[1], 4 - t[1])),
    )

    def norm_peer(n):
        dx, dz, dk = far_first[n]
        core = c if dk == 0 else other
        return core, mod4(x + dx) * 4 + mod4(z + dz)

    def d_norm(q, n):
        core, to_mp = norm_peer(n)
        return remote(nb.at[q, spot], nb.at[q, spot], sn.at[q, n], rn.at[q, spot], y * 2 + core, to_mp)

    def norm_send(q):
        col = jnp.sum(jnp.sum(npart[...], axis=1), axis=1, keepdims=True)
        nb[q, spot] = jnp.sum(jnp.where(l16 == r16, col, 0.0), axis=0, keepdims=True)
        for n in range(31):
            d_norm(q, n).start()

    def picked(table, index, shape):
        out = jnp.zeros(shape, F32)
        for n in range(4):
            out = out + jnp.where(index == n, table[n : n + 1], 0.0)
        return out

    def factor(squares):
        return clip_limit / jnp.maximum(jnp.sqrt(squares), clip_limit)

    def norm_take(q):
        for n in range(31):
            core, from_mp = norm_peer(n)
            ref = nb.at[q, core * 16 + from_mp]
            remote(ref, ref, sn.at[q, n], rn.at[q, core * 16 + from_mp], dp, mp).wait_recv()
        rows = nb[q].reshape(32, 128)
        s0 = rows[0:4] + rows[4:8] + rows[8:12] + rows[12:16]
        s1 = jnp.concatenate(
            [jnp.sum(rows[16 + 4 * n : 20 + 4 * n], axis=0, keepdims=True) for n in range(4)], axis=0
        )
        mine = jnp.where(c == 0, s0, s1)
        others = jnp.where(c == 0, s1, s0)
        place16, half16 = lax.rem(lax.div(r16, 2), 4), lax.rem(r16, 2)
        squares = jnp.sum(
            jnp.where(l16 == r16, picked(mine, a, (16, 128)), 0.0)
            + jnp.where(l16 == lax.div(r16, 8) * 8 + a * 2 + half16, picked(others, place16, (16, 128)), 0.0),
            axis=1, keepdims=True,
        )
        scaled_mask = mask * factor(squares)
        for e in range(16):
            ft[e] = scaled_mask[e : e + 1]
        return s0, s1

    for q in range(5):
        for s in (2, 0, 1):
            for cp in range(2):
                w_h(cp, s, q)
            if q < 3:
                loop(2, lambda cp: tiles(cp, mod4(q - a), mod4(a - STEPS[s])))
            else:
                for cp in range(2):
                    tiles(cp, mod4(3 - a), mod4(a - STEPS[s]), (q - 3,))
        if q == 2:
            norm_send(0)
    norm_send(1)
    norm_take(0)

    def owner(n):
        return mod4(a + 2 - n + 3 * (n // 2) - 2 * (n // 3))

    def products(m, ranks):
        total = None
        for r in ranks:
            for cp in range(2):
                for j in range(2):
                    i = mod4(r - a)
                    h = (hb[cp, i, j, m].astype(F32) * ft[cp * 8 + i * 2 + j]).astype(BF16)
                    p = jnp.dot(h, xb[cp, i, j], preferred_element_type=F32)
                    total = p if total is None else total + p
        return total

    def early(n):
        gall[n] = products(owner(n), (0, 1, 2))

    loop(4, early)
    s0, s1 = norm_take(1)

    def d_part(n):
        return remote(gs.at[n], gr.at[n], sg.at[n], rg.at[n], dp, mp_of(g, owner(n)))

    for n in range(4):
        m = owner(n)
        total = gall[n] + products(m, (3,))
        gh[pl.ds(pl.multiple_of(m * HIGH, HIGH), HIGH)] = total[LOW:]
        if n < 3:
            gs[n] = total[:LOW].astype(BF16)
            d_part(n).start()
        else:
            gall[n, :LOW] = total[:LOW]

    def d_y(src, dst, ssem, rsem, dy, k):
        to_dp = mod4(y + dy) * 2 + k
        return remote(src.at[to_dp], dst.at[c, dy], ssem.at[dy, k], rsem.at[c, dy], to_dp, mp)

    def d_partner(src, dst, ssem, rsem):
        to_dp = y * 2 + other
        return remote(src.at[to_dp], dst.at[c, 0], ssem.at[0, 0], rsem.at[c, 0], to_dp, mp)

    def y_start(*refs):
        for dy in (2, 1, 3):
            for k in range(2):
                d_y(*refs, dy, k).start()
        d_partner(*refs).start()

    def y_wait(src, dst, ssem, rsem):
        ref = dst.at[other, 0]
        remote(ref, ref, ssem.at[0, 1], rsem.at[other, 0], dp, mp).wait_recv()
        for dy in (1, 3, 2):
            for k in range(2):
                ref = dst.at[k, dy]
                remote(ref, ref, ssem.at[dy, k], rsem.at[k, dy], dp, mp).wait_recv()

    over_low, over_high = (ys, yr, sy, ry), (yhs, yhr, syh, ryh)
    turned = gh[...].T.astype(BF16)
    for b in range(8):
        yhs[b] = turned[b * OWN : (b + 1) * OWN]
    y_start(*over_high)
    yhr[c, 0] = yhs[dp]

    r32 = lax.broadcasted_iota(jnp.int32, (32, 128), 0)
    l32 = lax.broadcasted_iota(jnp.int32, (32, 128), 1)
    x32, z32, j32 = lax.div(r32, 8), lax.rem(lax.div(r32, 2), 4), lax.rem(r32, 2)
    squares = jnp.sum(
        jnp.where(l32 == c * 8 + x32 * 2 + j32, picked(s0, z32, (32, 128)), 0.0)
        + jnp.where(l32 == c * 8 + z32 * 2 + j32, picked(s1, x32, (32, 128)), 0.0),
        axis=1, keepdims=True,
    )
    clip_ref[...] = jnp.sum(
        jnp.where(l32[:, :32] == r32[:, :32], factor(squares), 0.0), axis=0, keepdims=True
    )

    for n in range(3):
        remote(gr.at[n], gr.at[n], sg.at[n], rg.at[n], dp, mp).wait_recv()
    low = gall[3, :LOW] + gr[0].astype(F32) + gr[1].astype(F32) + gr[2].astype(F32)
    turned = low.T.astype(BF16)
    for b in range(8):
        ys[b] = turned[b * OWN : (b + 1) * OWN]
    y_start(*over_low)
    yr[c, 0] = ys[dp]

    def d_high(k, s):
        gk, ak = place(k)
        aa = mod4(ak + STEPS[s])
        return remote(hs.at[k, lax.div(aa, 2)], hr.at[k, s], shh.at[k, s], rhh.at[k, s], dp, mp_k(k, gk, aa))

    y_wait(*over_high)
    for k in range(2):
        high = yhr[k, 0].astype(F32)
        for dy in range(1, 4):
            high = high + yhr[k, dy].astype(F32)
        for t in range(2):
            hs[k, t] = high[:, t * 128 : (t + 1) * 128].astype(BF16)
        for s in (2, 0, 1):
            d_high(k, s).start()
    total = jnp.dot(hs[0, lax.div(place(0)[1], 2)], eh[0], preferred_element_type=F32)
    total = total + jnp.dot(hs[1, lax.div(place(1)[1], 2)], eh[1], preferred_element_type=F32)
    y_wait(*over_low)
    for k in range(2):
        for dy in range(4):
            total = total + jnp.dot(yr[k, dy], eb[k], preferred_element_type=F32)
    for k in range(2):
        for s in (0, 1, 2):
            remote(hr.at[k, s], hr.at[k, s], shh.at[k, s], rhh.at[k, s], dp, mp).wait_recv()
            total = total + jnp.dot(hr[k, s], eh[k], preferred_element_type=F32)
    grad_ref[...] = total * (1.0 / EXAMPLES)

    d_len.wait_send()
    for k in range(2):
        @pl.when(c != k)
        def _():
            for d in d_own_remote(k):
                d.wait_send()
        for s in range(2):
            for j in range(2):
                d_x(k, s, j).wait_send()
            d_xf(k, s).wait_send()
        for s in range(3):
            for q in range(5):
                d_h(k, s, q).wait_send()
            d_high(k, s).wait_send()
    for q in range(2):
        for n in range(31):
            d_norm(q, n).wait_send()
    for n in range(3):
        d_part(n).wait_send()
    for refs in (over_low, over_high):
        for dy in (2, 1, 3):
            for k in range(2):
                d_y(*refs, dy, k).wait_send()
        d_partner(*refs).wait_send()


def exchange(layer_input, output_cot, hidden_cot, hidden_act, lengths):
    dma = pltpu.SemaphoreType.DMA
    hbm = pl.BlockSpec(memory_space=pltpu.HBM)
    vmem = pl.BlockSpec(memory_space=pltpu.VMEM)
    return pl.pallas_call(
        kernel,
        out_shape=(jax.ShapeDtypeStruct((OWN, 2 * ROWS), F32), jax.ShapeDtypeStruct((1, 32), F32)),
        in_specs=[hbm] * 5,
        out_specs=(vmem, vmem),
        scratch_shapes=[
            pltpu.VMEM((2, 4, 2, SLOT, D), BF16),
            pltpu.VMEM((2, 4, 2, 4, ROWS, SLOT), BF16),
            pltpu.VMEM((4, ROWS, D), F32),
            pltpu.VMEM((3, 128, D), BF16),
            pltpu.VMEM((3, 128, D), BF16),
            pltpu.VMEM((256, D), F32),
            pltpu.VMEM((8, OWN, 128), BF16),
            pltpu.VMEM((2, 4, OWN, 128), BF16),
            pltpu.VMEM((8, OWN, 256), BF16),
            pltpu.VMEM((2, 4, OWN, 256), BF16),
            pltpu.VMEM((2, 2, OWN, 128), BF16),
            pltpu.VMEM((2, 3, OWN, 128), BF16),
            pltpu.VMEM((2, 128, 2 * ROWS), BF16),
            pltpu.VMEM((2, 128, 2 * ROWS), BF16),
            pltpu.VMEM((2, 1, 32), jnp.int32),
            pltpu.VMEM((16, 1, SLOT), F32),
            pltpu.VMEM((16, 1, SLOT), F32),
            pltpu.VMEM((16, 8, 128), F32),
            pltpu.VMEM((2, 32, 1, 128), F32),
            dma((2,)), dma, dma((2, 2, 2)), dma, dma((2, 3, 5)), dma, dma, dma((2, 2)),
            dma((2, 31)), dma((3,)), dma((4, 2)), dma((4, 2)), dma((2, 3)),
            dma((2, 3, 2)), dma, dma((2, 3, 5)), dma, dma, dma((2, 32)), dma((3,)), dma((2, 4)), dma((2, 4)), dma((2, 3)),
            pltpu.SemaphoreType.REGULAR((3,)),
        ],
        compiler_params=pltpu.CompilerParams(has_side_effects=True, collective_id=0, vmem_limit_bytes=56_000_000),
    )(layer_input, output_cot, hidden_cot, hidden_act, lengths)


def local(
    layer_input, output_cot, hidden_act, hidden_cot, lengths, weights, moment_one, moment_two
):
    by_place = (4, 4, 2, ROWS, SLOT)
    gradient, clip = exchange(
        layer_input, output_cot, hidden_cot.reshape(by_place), hidden_act.reshape(by_place), lengths.reshape(1, 32)
    )
    new_moment_one = beta_one * moment_one + (1.0 - beta_one) * gradient
    new_moment_two = beta_two * moment_two + (1.0 - beta_two) * gradient * gradient
    corr_one = 1.0 - beta_one**STEP
    corr_two = 1.0 - beta_two**STEP
    direction = new_moment_one / corr_one / (jnp.sqrt(new_moment_two / corr_two) + adam_eps)
    new_weights = weights - learn_rate * (direction + weight_decay * weights)
    return (new_weights, new_moment_one, new_moment_two, clip.reshape(32))


def solution(mesh):
    return jax.shard_map(
        local,
        mesh=mesh,
        in_specs=(
            P(("dp", "mp"), None, None),
            P(("dp", "mp"), None, None),
            P("dp", "mp", None),
            P("dp", "mp", None),
            P("dp"),
            P("dp", "mp"),
            P("dp", "mp"),
            P("dp", "mp"),
        ),
        out_specs=(P("dp", "mp"), P("dp", "mp"), P("dp", "mp"), P("dp")),
        check_vma=False,
    )
```

```python
import math

import jax
import jax.numpy as jnp
from jax import lax
from jax.experimental import pallas as pl
from jax.experimental.pallas import tpu as pltpu
from jax.sharding import PartitionSpec as P

D = 768
FF = 3072
SLOT = 256
STEP = 10
EXAMPLES = 256
ROWS = 192
OWN = 96

beta_one = 0.9
beta_two = 0.999
adam_eps = 1e-08
learn_rate = 0.001
weight_decay = 0.01
clip_limit = 0.5 * math.sqrt(2.0 * D * FF * SLOT)

MESH = pl.DeviceIdType.MESH
BF16 = jnp.bfloat16
F32 = jnp.float32


def kernel(
    x0_ref, x1_ref, h0_ref, h1_ref, len_ref,
    grad_ref, clip_ref,
    xb, hb, gall, gs, gr, gh, ys, yr, yhs, yhr, hs, hr, eb, eh, lb, mt, ft, fc, npart, nb, p3,
    lsem, llen, sx, sxo, sh, sho, slen, sxf, sn, sg, sy, syh, shh,
    rx, rxo, rh, rho, rlen, rn, rg, ry, ryh, rhh, near,
):
    dp, mp = lax.axis_index("dp"), lax.axis_index("mp")
    c, y = lax.rem(dp, 2), lax.div(dp, 2)
    x, z = lax.div(mp, 4), lax.rem(mp, 4)
    other = 1 - c
    mod4 = lambda v: lax.rem(v + 8, 4)
    g = c * z + (1 - c) * x
    a = c * x + (1 - c) * z
    mp_of = lambda gg, aa: (1 - c) * (gg * 4 + aa) + c * (aa * 4 + gg)

    def remote(src, dst, ssem, rsem, to_dp, to_mp):
        return pltpu.make_async_remote_copy(
            src_ref=src, dst_ref=dst, send_sem=ssem, recv_sem=rsem,
            device_id={"dp": to_dp, "mp": to_mp}, device_id_type=MESH,
        )

    def signal(sem, to_dp, to_mp):
        pl.semaphore_signal(sem, inc=1, device_id={"dp": to_dp, "mp": to_mp}, device_id_type=MESH)

    def loop(count, body):
        lax.fori_loop(0, count, lambda n, carry: (body(n), carry)[1], 0)

    x_refs, h_refs = (x0_ref, x1_ref), (h0_ref, h1_ref)
    STEPS = (1, -1, 2)
    LOW, HIGH = 128, ROWS - 128

    def place(k):
        return (x, z) if k == 0 else (z, x)

    def mp_k(k, gg, aa):
        return gg * 4 + aa if k == 0 else aa * 4 + gg

    def h_slice(k, i, aa):
        return h_refs[k].at[i, aa] if k == 0 else h_refs[k].at[aa, i]

    def h_all(k, aa):
        return h_refs[k].at[:, aa] if k == 0 else h_refs[k].at[aa]

    def d_x(k, s, j):
        gk, ak = place(k)
        return remote(x_refs[k].at[j], xb.at[c, gk, j], sx.at[k, s, j], rx.at[c, s, j],
                      y * 2 + k, mp_k(k, mod4(gk + STEPS[s]), ak))

    def d_h(k, s, q):
        gk, ak = place(k)
        aa = mod4(ak + STEPS[s])
        i = mod4(min(q, 3) - aa)
        src, dst = h_slice(k, i, aa), hb.at[c, i, :, ak]
        if q >= 3:
            src, dst = src.at[q - 3], hb.at[c, i, q - 3, ak]
        return remote(src, dst, sh.at[k, s, q], rh.at[c, s, q], y * 2 + k, mp_k(k, gk, aa))

    def d_own_remote(k):
        gk, ak = place(k)
        return (
            remote(x_refs[k], xb.at[c, gk], sxo, rxo, y * 2 + k, mp),
            remote(h_all(k, ak), hb.at[c, :, :, ak], sho, rho, y * 2 + k, mp),
        )

    def d_own_local(k):
        gk, ak = place(k)
        return (
            pltpu.make_async_copy(x_refs[k], xb.at[c, gk], lsem.at[0]),
            pltpu.make_async_copy(h_all(k, ak), hb.at[c, :, :, ak], lsem.at[1]),
        )

    d_len = remote(len_ref, lb.at[c], slen, rlen, y * 2 + other, mp)
    d_len_local = pltpu.make_async_copy(len_ref, lb.at[c], llen)

    def d_xf(cp, s):
        src = xb.at[cp, mod4(g - STEPS[s]), s]
        return remote(src, src, sxf.at[cp, s], rx.at[cp, 2, s], dp, mp_of(mod4(g + STEPS[s]), a))

    def w_x(cp, s, j):
        ref = xb.at[cp, mod4(g - STEPS[s]), j]
        remote(ref, ref, sx.at[0, s, j], rx.at[cp, s, j], dp, mp).wait_recv()

    def w_xf(cp, s):
        ref = xb.at[cp, mod4(g + 2), s]
        remote(ref, ref, sxf.at[0, s], rx.at[cp, 2, s], dp, mp).wait_recv()

    def w_h(cp, s, q):
        half = slice(None) if q < 3 else q - 3
        ref = hb.at[cp, mod4(min(q, 3) - a), half, mod4(a - STEPS[s])]
        remote(ref, ref, sh.at[0, s, q], rh.at[cp, s, q], dp, mp).wait_recv()

    in_x = [mod4(x + s) * 4 + z for s in STEPS[:2]]
    in_z = [x * 4 + mod4(z + s) for s in STEPS[:2]]
    in_y = [mod4(y + s) * 2 for s in STEPS[:2]]
    barrier = pltpu.get_barrier_semaphore()
    signal(barrier, y * 2 + other, mp)
    for k in range(2):
        for to_mp in in_x + in_z:
            signal(barrier, y * 2 + k, to_mp)
        for to_dp in in_y:
            signal(barrier, to_dp + k, mp)
    pl.semaphore_wait(barrier, 13)

    for q in range(2):
        for k in range(2):
            for s in range(2):
                d_x(k, s, q if s == 0 else 1 - q).start()
    d_len_local.start()
    d_len.start()
    for k in range(2):
        @pl.when(c == k)
        def _():
            for d in d_own_local(k):
                d.start()

        @pl.when(c != k)
        def _():
            for d in d_own_remote(k):
                d.start()
    for to_mp in in_x + in_z:
        signal(near.at[0], dp, to_mp)
    for to_dp in in_y:
        signal(near.at[0], to_dp + c, mp)

    f_row = lax.broadcasted_iota(jnp.int32, (128, 2 * ROWS), 0)
    column = lax.broadcasted_iota(jnp.int32, (128, 2 * ROWS), 1)
    for k in range(2):
        eb[k] = jnp.where(column == 2 * f_row + k, 1.0, 0.0).astype(BF16)
        high = f_row - HIGH * lax.rem(place(k)[1], 2)
        hit = jnp.where(column == 2 * (LOW + high) + k, 1.0, 0.0)
        eh[k] = jnp.where(high < HIGH, jnp.where(high >= 0, hit, 0.0), 0.0).astype(BF16)
    npart[...] = jnp.zeros_like(npart)

    d_len_local.wait()
    d_len.wait_recv()
    e_row = lax.broadcasted_iota(jnp.int32, (16, 32), 0)
    e_lane = lax.broadcasted_iota(jnp.int32, (16, 32), 1)
    e_place, e_half = lax.rem(lax.div(e_row, 2), 4), lax.rem(e_row, 2)
    wanted = mp_of(e_place, a) * 2 + e_half
    lens = jnp.where(e_row < 8, lb[0], lb[1]).astype(F32)
    len_col = jnp.sum(jnp.where(e_lane == wanted, lens, 0.0), axis=1, keepdims=True)
    slot = lax.broadcasted_iota(jnp.int32, (16, SLOT), 1).astype(F32)
    mask = jnp.where(slot < len_col, 1.0, 0.0)
    for e in range(16):
        mt[e] = mask[e : e + 1]

    def masked_product(cp, i, j, m):
        h = hb[cp, i, j, m] * mt[cp * 8 + i * 2 + j].astype(BF16)
        return jnp.dot(h, xb[cp, i, j], preferred_element_type=F32)

    def tiles(cp, i, m, halves=(0, 1), keep=False):
        for j in halves:
            e = cp * 8 + i * 2 + j
            p = masked_product(cp, i, j, m)
            if keep:
                p3[cp, j, m] = p
            p = jnp.sum((p * p).reshape(ROWS // 8, 8, D), axis=0)
            part = p[:, :128]
            for n in range(1, D // 128):
                part = part + p[:, n * 128 : (n + 1) * 128]
            npart[e] += part

    for cp in range(2):
        for s in range(2):
            w_x(cp, s, s)
            d_xf(cp, s).start()
    pl.semaphore_wait(near.at[0], 6)
    def send_rank(*parts):
        for q in parts:
            for s in (2, 0, 1):
                for k in range(2):
                    d_h(k, s, q).start()

    send_rank(0, 1, 2)
    for to_mp in in_z:
        signal(near.at[1], dp, to_mp)

    for k in range(2):
        @pl.when(c == k)
        def _():
            for d in d_own_local(k):
                d.wait()
    own_x, own_h = xb.at[other, g], hb.at[other, :, :, a]
    remote(own_x, own_x, sxo, rxo, dp, mp).wait_recv()
    remote(own_h, own_h, sho, rho, dp, mp).wait_recv()
    loop(2, lambda cp: tiles(cp, g, a))
    for cp in range(2):
        for s in range(2):
            w_x(cp, s, 1 - s)
    loop(4, lambda n: tiles(lax.div(n, 2), mod4(g + 1 + 2 * lax.rem(n, 2)), a))
    pl.semaphore_wait(near.at[1], 2)
    for to_mp in in_z:
        signal(near.at[2], dp, to_mp)
    for cp in range(2):
        for s in range(2):
            w_xf(cp, s)
    loop(2, lambda cp: tiles(cp, mod4(g + 2), a))
    for cp in range(2):
        for j in range(2):
            p3[cp, j, a] = masked_product(cp, mod4(3 - a), j, a)
    pl.semaphore_wait(near.at[2], 2)

    spot = c * 16 + mp
    r16 = lax.broadcasted_iota(jnp.int32, (16, 128), 0)
    l16 = lax.broadcasted_iota(jnp.int32, (16, 128), 1)
    far_first = sorted(
        [(dx, dz, dk) for dx in range(4) for dz in range(4) for dk in range(2) if dx or dz or dk],
        key=lambda t: -(min(t[0], 4 - t[0]) + min(t[1], 4 - t[1])),
    )

    def norm_peer(n):
        dx, dz, dk = far_first[n]
        core = c if dk == 0 else other
        return core, mod4(x + dx) * 4 + mod4(z + dz)

    def d_norm(q, n):
        core, to_mp = norm_peer(n)
        return remote(nb.at[q, spot], nb.at[q, spot], sn.at[q, n], rn.at[q, spot], y * 2 + core, to_mp)

    def norm_send(q):
        col = jnp.sum(jnp.sum(npart[...], axis=1), axis=1, keepdims=True)
        nb[q, spot] = jnp.sum(jnp.where(l16 == r16, col, 0.0), axis=0, keepdims=True)
        for n in range(31):
            d_norm(q, n).start()

    def picked(table, index, shape):
        out = jnp.zeros(shape, F32)
        for n in range(4):
            out = out + jnp.where(index == n, table[n : n + 1], 0.0)
        return out

    def factor(squares):
        return clip_limit / jnp.maximum(jnp.sqrt(squares), clip_limit)

    def norm_take(q):
        for n in range(31):
            core, from_mp = norm_peer(n)
            ref = nb.at[q, core * 16 + from_mp]
            remote(ref, ref, sn.at[q, n], rn.at[q, core * 16 + from_mp], dp, mp).wait_recv()
        rows = nb[q].reshape(32, 128)
        s0 = rows[0:4] + rows[4:8] + rows[8:12] + rows[12:16]
        s1 = jnp.concatenate(
            [jnp.sum(rows[16 + 4 * n : 20 + 4 * n], axis=0, keepdims=True) for n in range(4)], axis=0
        )
        mine = jnp.where(c == 0, s0, s1)
        others = jnp.where(c == 0, s1, s0)
        place16, half16 = lax.rem(lax.div(r16, 2), 4), lax.rem(r16, 2)
        squares = jnp.sum(
            jnp.where(l16 == r16, picked(mine, a, (16, 128)), 0.0)
            + jnp.where(l16 == lax.div(r16, 8) * 8 + a * 2 + half16, picked(others, place16, (16, 128)), 0.0),
            axis=1, keepdims=True,
        )
        scale = factor(squares)
        if q == 2:
            for e in range(16):
                fc[e] = jnp.broadcast_to(scale[e : e + 1], (1, D))
        else:
            scaled_mask = mask * scale
            for e in range(16):
                ft[e] = scaled_mask[e : e + 1]
        return s0, s1

    def owner(n):
        return mod4(a + 2 - n + 3 * (n // 2) - 2 * (n // 3))

    def products(m, ranks):
        total = None
        for r in ranks:
            for cp in range(2):
                for j in range(2):
                    i = mod4(r - a)
                    h = (hb[cp, i, j, m].astype(F32) * ft[cp * 8 + i * 2 + j]).astype(BF16)
                    p = jnp.dot(h, xb[cp, i, j], preferred_element_type=F32)
                    total = p if total is None else total + p
        return total

    def early(n):
        gall[n] = products(owner(n), (0, 1))

    def third(n):
        gall[n] += products(owner(n), (2,))

    for q in range(5):
        for s in (2, 0, 1):
            for cp in range(2):
                w_h(cp, s, q)
            if q < 3:
                loop(2, lambda cp: tiles(cp, mod4(q - a), mod4(a - STEPS[s])))
            else:
                for cp in range(2):
                    tiles(cp, mod4(3 - a), mod4(a - STEPS[s]), (q - 3,), True)
        if q in (1, 2):
            norm_send(q - 1)
        if q == 1:
            send_rank(3, 4)
        if q == 2:
            norm_take(0)
            loop(4, early)
    norm_send(2)
    norm_take(1)
    loop(4, third)
    s0, s1 = norm_take(2)

    def d_part(n):
        return remote(gs.at[n], gr.at[n], sg.at[n], rg.at[n], dp, mp_of(g, owner(n)))

    def final_rows(n, row):
        rows = pl.ds(row, 16)
        total = gall[n, rows]
        for cp in range(2):
            for j in range(2):
                total = total + fc[cp * 8 + mod4(3 - a) * 2 + j] * p3[cp, j, owner(n), rows]
        return total

    for n in range(4):
        for row in range(0, LOW, 16):
            if n < 3:
                gs[n, row : row + 16] = final_rows(n, row).astype(BF16)
            else:
                gall[n, row : row + 16] = final_rows(n, row)
        if n < 3:
            d_part(n).start()
        for row in range(LOW, ROWS, 16):
            gh[pl.ds(pl.multiple_of(owner(n) * HIGH + row - LOW, 16), 16)] = final_rows(n, row)

    def d_y(src, dst, ssem, rsem, dy, k):
        to_dp = mod4(y + dy) * 2 + k
        return remote(src.at[to_dp], dst.at[c, dy], ssem.at[dy, k], rsem.at[c, dy], to_dp, mp)

    def d_partner(src, dst, ssem, rsem):
        to_dp = y * 2 + other
        return remote(src.at[to_dp], dst.at[c, 0], ssem.at[0, 0], rsem.at[c, 0], to_dp, mp)

    def y_start(*refs):
        for dy in (2, 1, 3):
            for k in range(2):
                d_y(*refs, dy, k).start()
        d_partner(*refs).start()

    def y_wait(src, dst, ssem, rsem):
        ref = dst.at[other, 0]
        remote(ref, ref, ssem.at[0, 1], rsem.at[other, 0], dp, mp).wait_recv()
        for dy in (1, 3, 2):
            for k in range(2):
                ref = dst.at[k, dy]
                remote(ref, ref, ssem.at[dy, k], rsem.at[k, dy], dp, mp).wait_recv()

    over_low, over_high = (ys, yr, sy, ry), (yhs, yhr, syh, ryh)
    turned = gh[...].T.astype(BF16)
    for b in range(8):
        yhs[b] = turned[b * OWN : (b + 1) * OWN]
    y_start(*over_high)
    yhr[c, 0] = yhs[dp]

    r32 = lax.broadcasted_iota(jnp.int32, (32, 128), 0)
    l32 = lax.broadcasted_iota(jnp.int32, (32, 128), 1)
    x32, z32, j32 = lax.div(r32, 8), lax.rem(lax.div(r32, 2), 4), lax.rem(r32, 2)
    squares = jnp.sum(
        jnp.where(l32 == c * 8 + x32 * 2 + j32, picked(s0, z32, (32, 128)), 0.0)
        + jnp.where(l32 == c * 8 + z32 * 2 + j32, picked(s1, x32, (32, 128)), 0.0),
        axis=1, keepdims=True,
    )
    clip_ref[...] = jnp.sum(
        jnp.where(l32[:, :32] == r32[:, :32], factor(squares), 0.0), axis=0, keepdims=True
    )

    for n in range(3):
        remote(gr.at[n], gr.at[n], sg.at[n], rg.at[n], dp, mp).wait_recv()
    low = gall[3, :LOW] + gr[0].astype(F32) + gr[1].astype(F32) + gr[2].astype(F32)
    turned = low.T.astype(BF16)
    for b in range(8):
        ys[b] = turned[b * OWN : (b + 1) * OWN]
    y_start(*over_low)
    yr[c, 0] = ys[dp]

    def d_high(k, s):
        gk, ak = place(k)
        aa = mod4(ak + STEPS[s])
        return remote(hs.at[k, lax.div(aa, 2)], hr.at[k, s], shh.at[k, s], rhh.at[k, s], dp, mp_k(k, gk, aa))

    y_wait(*over_high)
    for k in range(2):
        high = yhr[k, 0].astype(F32)
        for dy in range(1, 4):
            high = high + yhr[k, dy].astype(F32)
        for t in range(2):
            hs[k, t] = high[:, t * 128 : (t + 1) * 128].astype(BF16)
        for s in (2, 0, 1):
            d_high(k, s).start()
    total = jnp.dot(hs[0, lax.div(place(0)[1], 2)], eh[0], preferred_element_type=F32)
    total = total + jnp.dot(hs[1, lax.div(place(1)[1], 2)], eh[1], preferred_element_type=F32)
    y_wait(*over_low)
    for k in range(2):
        for dy in range(4):
            total = total + jnp.dot(yr[k, dy], eb[k], preferred_element_type=F32)
    for k in range(2):
        for s in (0, 1, 2):
            remote(hr.at[k, s], hr.at[k, s], shh.at[k, s], rhh.at[k, s], dp, mp).wait_recv()
            total = total + jnp.dot(hr[k, s], eh[k], preferred_element_type=F32)
    grad_ref[...] = total * (1.0 / EXAMPLES)

    d_len.wait_send()
    for k in range(2):
        @pl.when(c != k)
        def _():
            for d in d_own_remote(k):
                d.wait_send()
        for s in range(2):
            for j in range(2):
                d_x(k, s, j).wait_send()
            d_xf(k, s).wait_send()
        for s in range(3):
            for q in range(5):
                d_h(k, s, q).wait_send()
            d_high(k, s).wait_send()
    for q in range(3):
        for n in range(31):
            d_norm(q, n).wait_send()
    for n in range(3):
        d_part(n).wait_send()
    for refs in (over_low, over_high):
        for dy in (2, 1, 3):
            for k in range(2):
                d_y(*refs, dy, k).wait_send()
        d_partner(*refs).wait_send()


def exchange(layer_input, output_cot, hidden_cot, hidden_act, lengths):
    dma = pltpu.SemaphoreType.DMA
    hbm = pl.BlockSpec(memory_space=pltpu.HBM)
    vmem = pl.BlockSpec(memory_space=pltpu.VMEM)
    return pl.pallas_call(
        kernel,
        out_shape=(jax.ShapeDtypeStruct((OWN, 2 * ROWS), F32), jax.ShapeDtypeStruct((1, 32), F32)),
        in_specs=[hbm] * 5,
        out_specs=(vmem, vmem),
        scratch_shapes=[
            pltpu.VMEM((2, 4, 2, SLOT, D), BF16),
            pltpu.VMEM((2, 4, 2, 4, ROWS, SLOT), BF16),
            pltpu.VMEM((4, ROWS, D), F32),
            pltpu.VMEM((3, 128, D), BF16),
            pltpu.VMEM((3, 128, D), BF16),
            pltpu.VMEM((256, D), F32),
            pltpu.VMEM((8, OWN, 128), BF16),
            pltpu.VMEM((2, 4, OWN, 128), BF16),
            pltpu.VMEM((8, OWN, 256), BF16),
            pltpu.VMEM((2, 4, OWN, 256), BF16),
            pltpu.VMEM((2, 2, OWN, 128), BF16),
            pltpu.VMEM((2, 3, OWN, 128), BF16),
            pltpu.VMEM((2, 128, 2 * ROWS), BF16),
            pltpu.VMEM((2, 128, 2 * ROWS), BF16),
            pltpu.VMEM((2, 1, 32), jnp.int32),
            pltpu.VMEM((16, 1, SLOT), F32),
            pltpu.VMEM((16, 1, SLOT), F32),
            pltpu.VMEM((16, 1, D), F32),
            pltpu.VMEM((16, 8, 128), F32),
            pltpu.VMEM((3, 32, 1, 128), F32),
            pltpu.VMEM((2, 2, 4, ROWS, D), F32),
            dma((2,)), dma, dma((2, 2, 2)), dma, dma((2, 3, 5)), dma, dma, dma((2, 2)),
            dma((3, 31)), dma((3,)), dma((4, 2)), dma((4, 2)), dma((2, 3)),
            dma((2, 3, 2)), dma, dma((2, 3, 5)), dma, dma, dma((3, 32)), dma((3,)), dma((2, 4)), dma((2, 4)), dma((2, 3)),
            pltpu.SemaphoreType.REGULAR((3,)),
        ],
        compiler_params=pltpu.CompilerParams(has_side_effects=True, collective_id=0, vmem_limit_bytes=56_000_000),
    )(layer_input, output_cot, hidden_cot, hidden_act, lengths)


def local(
    layer_input, output_cot, hidden_act, hidden_cot, lengths, weights, moment_one, moment_two
):
    by_place = (4, 4, 2, ROWS, SLOT)
    gradient, clip = exchange(
        layer_input, output_cot, hidden_cot.reshape(by_place), hidden_act.reshape(by_place), lengths.reshape(1, 32)
    )
    new_moment_one = beta_one * moment_one + (1.0 - beta_one) * gradient
    new_moment_two = beta_two * moment_two + (1.0 - beta_two) * gradient * gradient
    corr_one = 1.0 - beta_one**STEP
    corr_two = 1.0 - beta_two**STEP
    direction = new_moment_one / corr_one / (jnp.sqrt(new_moment_two / corr_two) + adam_eps)
    new_weights = weights - learn_rate * (direction + weight_decay * weights)
    return (new_weights, new_moment_one, new_moment_two, clip.reshape(32))


def solution(mesh):
    return jax.shard_map(
        local,
        mesh=mesh,
        in_specs=(
            P(("dp", "mp"), None, None),
            P(("dp", "mp"), None, None),
            P("dp", "mp", None),
            P("dp", "mp", None),
            P("dp"),
            P("dp", "mp"),
            P("dp", "mp"),
            P("dp", "mp"),
        ),
        out_specs=(P("dp", "mp"), P("dp", "mp"), P("dp", "mp"), P("dp")),
        check_vma=False,
    )
```

```python
import math

import jax
import jax.numpy as jnp
from jax import lax
from jax.experimental import pallas as pl
from jax.experimental.pallas import tpu as pltpu
from jax.sharding import PartitionSpec as P

D = 768
FF = 3072
SLOT = 256
STEP = 10
EXAMPLES = 256
ROWS = 192
OWN = 96

beta_one = 0.9
beta_two = 0.999
adam_eps = 1e-08
learn_rate = 0.001
weight_decay = 0.01
clip_limit = 0.5 * math.sqrt(2.0 * D * FF * SLOT)

MESH = pl.DeviceIdType.MESH
BF16 = jnp.bfloat16
F32 = jnp.float32


def kernel(
    x0_ref, x1_ref, h0_ref, h1_ref, len_ref,
    grad_ref, clip_ref,
    xb, hb, gall, gs, gr, gh, ys, yr, yhs, yhr, hs, hr, eb, eh, lb, mt, ft, fc, npart, nb, p3,
    lsem, llen, sx, sxo, sh, sho, slen, sxf, sn, sg, sy, syh, shh,
    rx, rxo, rh, rho, rlen, rn, rg, ry, ryh, rhh, near,
):
    dp, mp = lax.axis_index("dp"), lax.axis_index("mp")
    c, y = lax.rem(dp, 2), lax.div(dp, 2)
    x, z = lax.div(mp, 4), lax.rem(mp, 4)
    other = 1 - c
    mod4 = lambda v: lax.rem(v + 8, 4)
    g = c * z + (1 - c) * x
    a = c * x + (1 - c) * z
    mp_of = lambda gg, aa: (1 - c) * (gg * 4 + aa) + c * (aa * 4 + gg)

    def remote(src, dst, ssem, rsem, to_dp, to_mp):
        return pltpu.make_async_remote_copy(
            src_ref=src, dst_ref=dst, send_sem=ssem, recv_sem=rsem,
            device_id={"dp": to_dp, "mp": to_mp}, device_id_type=MESH,
        )

    def signal(sem, to_dp, to_mp):
        pl.semaphore_signal(sem, inc=1, device_id={"dp": to_dp, "mp": to_mp}, device_id_type=MESH)

    def loop(count, body):
        lax.fori_loop(0, count, lambda n, carry: (body(n), carry)[1], 0)

    x_refs, h_refs = (x0_ref, x1_ref), (h0_ref, h1_ref)
    STEPS = (1, -1, 2)
    LOW, HIGH = 128, ROWS - 128

    def place(k):
        return (x, z) if k == 0 else (z, x)

    def mp_k(k, gg, aa):
        return gg * 4 + aa if k == 0 else aa * 4 + gg

    def h_slice(k, i, aa):
        return h_refs[k].at[i, aa] if k == 0 else h_refs[k].at[aa, i]

    def h_all(k, aa):
        return h_refs[k].at[:, aa] if k == 0 else h_refs[k].at[aa]

    def d_x(k, s, j):
        gk, ak = place(k)
        return remote(x_refs[k].at[j], xb.at[c, gk, j], sx.at[k, s, j], rx.at[c, s, j],
                      y * 2 + k, mp_k(k, mod4(gk + STEPS[s]), ak))

    def d_h(k, s, q):
        gk, ak = place(k)
        aa = mod4(ak + STEPS[s])
        i = mod4(min(q, 3) - aa)
        src, dst = h_slice(k, i, aa), hb.at[c, i, :, ak]
        if q >= 3:
            src, dst = src.at[q - 3], hb.at[c, i, q - 3, ak]
        return remote(src, dst, sh.at[k, s, q], rh.at[c, s, q], y * 2 + k, mp_k(k, gk, aa))

    def d_own_remote(k):
        gk, ak = place(k)
        return (
            remote(x_refs[k], xb.at[c, gk], sxo, rxo, y * 2 + k, mp),
            remote(h_all(k, ak), hb.at[c, :, :, ak], sho, rho, y * 2 + k, mp),
        )

    def d_own_local(k):
        gk, ak = place(k)
        return (
            pltpu.make_async_copy(x_refs[k], xb.at[c, gk], lsem.at[0]),
            pltpu.make_async_copy(h_all(k, ak), hb.at[c, :, :, ak], lsem.at[1]),
        )

    d_len = remote(len_ref, lb.at[c], slen, rlen, y * 2 + other, mp)
    d_len_local = pltpu.make_async_copy(len_ref, lb.at[c], llen)

    def d_xf(cp, s):
        src = xb.at[cp, mod4(g - STEPS[s]), s]
        return remote(src, src, sxf.at[cp, s], rx.at[cp, 2, s], dp, mp_of(mod4(g + STEPS[s]), a))

    def w_x(cp, s, j):
        ref = xb.at[cp, mod4(g - STEPS[s]), j]
        remote(ref, ref, sx.at[0, s, j], rx.at[cp, s, j], dp, mp).wait_recv()

    def w_xf(cp, s):
        ref = xb.at[cp, mod4(g + 2), s]
        remote(ref, ref, sxf.at[0, s], rx.at[cp, 2, s], dp, mp).wait_recv()

    def w_h(cp, s, q):
        half = slice(None) if q < 3 else q - 3
        ref = hb.at[cp, mod4(min(q, 3) - a), half, mod4(a - STEPS[s])]
        remote(ref, ref, sh.at[0, s, q], rh.at[cp, s, q], dp, mp).wait_recv()

    in_x = [mod4(x + s) * 4 + z for s in STEPS[:2]]
    in_z = [x * 4 + mod4(z + s) for s in STEPS[:2]]
    in_y = [mod4(y + s) * 2 for s in STEPS[:2]]
    barrier = pltpu.get_barrier_semaphore()
    signal(barrier, y * 2 + other, mp)
    for k in range(2):
        for to_mp in in_x + in_z:
            signal(barrier, y * 2 + k, to_mp)
        for to_dp in in_y:
            signal(barrier, to_dp + k, mp)
    pl.semaphore_wait(barrier, 13)

    for q in range(2):
        for k in range(2):
            for s in range(2):
                d_x(k, s, q if s == 0 else 1 - q).start()
    d_len_local.start()
    d_len.start()
    for k in range(2):
        @pl.when(c == k)
        def _():
            for d in d_own_local(k):
                d.start()

        @pl.when(c != k)
        def _():
            for d in d_own_remote(k):
                d.start()
    for to_mp in in_x + in_z:
        signal(near.at[0], dp, to_mp)
    for to_dp in in_y:
        signal(near.at[0], to_dp + c, mp)

    f_row = lax.broadcasted_iota(jnp.int32, (128, 2 * ROWS), 0)
    column = lax.broadcasted_iota(jnp.int32, (128, 2 * ROWS), 1)
    for k in range(2):
        eb[k] = jnp.where(column == 2 * f_row + k, 1.0, 0.0).astype(BF16)
        high = f_row - HIGH * lax.rem(place(k)[1], 2)
        hit = jnp.where(column == 2 * (LOW + high) + k, 1.0, 0.0)
        eh[k] = jnp.where(high < HIGH, jnp.where(high >= 0, hit, 0.0), 0.0).astype(BF16)
    npart[...] = jnp.zeros_like(npart)

    d_len_local.wait()
    d_len.wait_recv()
    e_row = lax.broadcasted_iota(jnp.int32, (16, 32), 0)
    e_lane = lax.broadcasted_iota(jnp.int32, (16, 32), 1)
    e_place, e_half = lax.rem(lax.div(e_row, 2), 4), lax.rem(e_row, 2)
    wanted = mp_of(e_place, a) * 2 + e_half
    lens = jnp.where(e_row < 8, lb[0], lb[1]).astype(F32)
    len_col = jnp.sum(jnp.where(e_lane == wanted, lens, 0.0), axis=1, keepdims=True)
    slot = lax.broadcasted_iota(jnp.int32, (16, SLOT), 1).astype(F32)
    mask = jnp.where(slot < len_col, 1.0, 0.0)
    for e in range(16):
        mt[e] = mask[e : e + 1]

    def masked_product(cp, i, j, m):
        h = hb[cp, i, j, m] * mt[cp * 8 + i * 2 + j].astype(BF16)
        return jnp.dot(h, xb[cp, i, j], preferred_element_type=F32)

    def tiles(cp, i, m, halves=(0, 1), keep=False):
        for j in halves:
            e = cp * 8 + i * 2 + j
            p = masked_product(cp, i, j, m)
            if keep:
                p3[cp, j, m] = p
            p = jnp.sum((p * p).reshape(ROWS // 8, 8, D), axis=0)
            part = p[:, :128]
            for n in range(1, D // 128):
                part = part + p[:, n * 128 : (n + 1) * 128]
            npart[e] += part

    for cp in range(2):
        for s in range(2):
            w_x(cp, s, s)
            d_xf(cp, s).start()
    pl.semaphore_wait(near.at[0], 6)
    def send_rank(*parts):
        for q in parts:
            for s in (2, 0, 1):
                for k in range(2):
                    d_h(k, s, q).start()

    send_rank(0, 1, 2)
    for to_mp in in_z:
        signal(near.at[1], dp, to_mp)

    for k in range(2):
        @pl.when(c == k)
        def _():
            for d in d_own_local(k):
                d.wait()
    own_x, own_h = xb.at[other, g], hb.at[other, :, :, a]
    remote(own_x, own_x, sxo, rxo, dp, mp).wait_recv()
    remote(own_h, own_h, sho, rho, dp, mp).wait_recv()
    loop(2, lambda cp: tiles(cp, g, a))
    for cp in range(2):
        for s in range(2):
            w_x(cp, s, 1 - s)
    loop(4, lambda n: tiles(lax.div(n, 2), mod4(g + 1 + 2 * lax.rem(n, 2)), a))
    pl.semaphore_wait(near.at[1], 2)
    for to_mp in in_z:
        signal(near.at[2], dp, to_mp)
    for cp in range(2):
        for s in range(2):
            w_xf(cp, s)
    loop(2, lambda cp: tiles(cp, mod4(g + 2), a))
    for cp in range(2):
        for j in range(2):
            p3[cp, j, a] = masked_product(cp, mod4(3 - a), j, a)
    pl.semaphore_wait(near.at[2], 2)

    spot = c * 16 + mp
    r16 = lax.broadcasted_iota(jnp.int32, (16, 128), 0)
    l16 = lax.broadcasted_iota(jnp.int32, (16, 128), 1)
    far_first = sorted(
        [(dx, dz) for dx in range(4) for dz in range(4)],
        key=lambda t: -(min(t[0], 4 - t[0]) + min(t[1], 4 - t[1])),
    )
    same_core = [(2, 0), (1, 0), (3, 0)] + [(dg, da) for da in (2, 1, 3) for dg in range(4)]
    NEEDED, ALL = 19, 31

    def norm_peer(n):
        if n < 16:
            dx, dz = far_first[n]
            return other, mod4(x + dx) * 4 + mod4(z + dz)
        dg, da = same_core[n - 16]
        return c, mp_of(mod4(g + dg), mod4(a + da))

    def d_norm(q, n):
        core, to_mp = norm_peer(n)
        return remote(nb.at[q, spot], nb.at[q, spot], sn.at[q, n], rn.at[q, spot], y * 2 + core, to_mp)

    def norm_send(q):
        col = jnp.sum(jnp.sum(npart[...], axis=1), axis=1, keepdims=True)
        nb[q, spot] = jnp.sum(jnp.where(l16 == r16, col, 0.0), axis=0, keepdims=True)
        for n in range(NEEDED):
            d_norm(q, n).start()

    def picked(table, index, shape):
        out = jnp.zeros(shape, F32)
        for n in range(4):
            out = out + jnp.where(index == n, table[n : n + 1], 0.0)
        return out

    def factor(squares):
        return clip_limit / jnp.maximum(jnp.sqrt(squares), clip_limit)

    def norm_wait(q, first, last):
        for n in range(first, last):
            core, from_mp = norm_peer(n)
            ref = nb.at[q, core * 16 + from_mp]
            remote(ref, ref, sn.at[q, n], rn.at[q, core * 16 + from_mp], dp, mp).wait_recv()

    def over_x(rows):
        return rows[0:4] + rows[4:8] + rows[8:12] + rows[12:16]

    def over_z(rows):
        return jnp.concatenate(
            [jnp.sum(rows[4 * n : 4 * n + 4], axis=0, keepdims=True) for n in range(4)], axis=0
        )

    def norm_take(q):
        norm_wait(q, 0, NEEDED)
        rows = nb[q, pl.ds(other * 16, 16)].reshape(16, 128)
        others = jnp.where(c == 0, over_z(rows), over_x(rows))
        mine = nb[q, c * 16 + mp_of(0, a)]
        for n in range(1, 4):
            mine = mine + nb[q, c * 16 + mp_of(n, a)]
        place16, half16 = lax.rem(lax.div(r16, 2), 4), lax.rem(r16, 2)
        squares = jnp.sum(
            jnp.where(l16 == r16, mine, 0.0)
            + jnp.where(l16 == lax.div(r16, 8) * 8 + a * 2 + half16, picked(others, place16, (16, 128)), 0.0),
            axis=1, keepdims=True,
        )
        scale = factor(squares)
        if q == 2:
            for e in range(16):
                fc[e] = jnp.broadcast_to(scale[e : e + 1], (1, D))
        else:
            scaled_mask = mask * scale
            for e in range(16):
                ft[e] = scaled_mask[e : e + 1]

    def owner(n):
        return mod4(a + 2 - n + 3 * (n // 2) - 2 * (n // 3))

    def products(m, ranks):
        total = None
        for r in ranks:
            for cp in range(2):
                for j in range(2):
                    i = mod4(r - a)
                    h = (hb[cp, i, j, m].astype(F32) * ft[cp * 8 + i * 2 + j]).astype(BF16)
                    p = jnp.dot(h, xb[cp, i, j], preferred_element_type=F32)
                    total = p if total is None else total + p
        return total

    def early(n):
        gall[n] = products(owner(n), (0, 1))

    def third(n):
        gall[n] += products(owner(n), (2,))

    for q in range(5):
        for s in (2, 0, 1):
            for cp in range(2):
                w_h(cp, s, q)
            if q < 3:
                loop(2, lambda cp: tiles(cp, mod4(q - a), mod4(a - STEPS[s])))
            else:
                for cp in range(2):
                    tiles(cp, mod4(3 - a), mod4(a - STEPS[s]), (q - 3,), True)
        if q in (1, 2):
            norm_send(q - 1)
        if q == 1:
            send_rank(3, 4)
        if q == 2:
            norm_take(0)
            loop(4, early)
    norm_send(2)
    norm_take(1)
    loop(4, third)
    norm_take(2)

    def d_part(n):
        return remote(gs.at[n], gr.at[n], sg.at[n], rg.at[n], dp, mp_of(g, owner(n)))

    def final_rows(n, row):
        rows = pl.ds(row, 16)
        total = gall[n, rows]
        for cp in range(2):
            for j in range(2):
                total = total + fc[cp * 8 + mod4(3 - a) * 2 + j] * p3[cp, j, owner(n), rows]
        return total

    for n in range(4):
        for row in range(0, LOW, 16):
            if n < 3:
                gs[n, row : row + 16] = final_rows(n, row).astype(BF16)
            else:
                gall[n, row : row + 16] = final_rows(n, row)
        if n < 3:
            d_part(n).start()
        for row in range(LOW, ROWS, 16):
            gh[pl.ds(pl.multiple_of(owner(n) * HIGH + row - LOW, 16), 16)] = final_rows(n, row)

    def d_y(src, dst, ssem, rsem, dy, k):
        to_dp = mod4(y + dy) * 2 + k
        return remote(src.at[to_dp], dst.at[c, dy], ssem.at[dy, k], rsem.at[c, dy], to_dp, mp)

    def d_partner(src, dst, ssem, rsem):
        to_dp = y * 2 + other
        return remote(src.at[to_dp], dst.at[c, 0], ssem.at[0, 0], rsem.at[c, 0], to_dp, mp)

    def y_start(*refs):
        for dy in (2, 1, 3):
            for k in range(2):
                d_y(*refs, dy, k).start()
        d_partner(*refs).start()

    def y_wait(src, dst, ssem, rsem):
        ref = dst.at[other, 0]
        remote(ref, ref, ssem.at[0, 1], rsem.at[other, 0], dp, mp).wait_recv()
        for dy in (1, 3, 2):
            for k in range(2):
                ref = dst.at[k, dy]
                remote(ref, ref, ssem.at[dy, k], rsem.at[k, dy], dp, mp).wait_recv()

    over_low, over_high = (ys, yr, sy, ry), (yhs, yhr, syh, ryh)
    for n in range(NEEDED, ALL):
        d_norm(2, n).start()
    turned = gh[...].T.astype(BF16)
    for b in range(8):
        yhs[b] = turned[b * OWN : (b + 1) * OWN]
    y_start(*over_high)
    yhr[c, 0] = yhs[dp]

    for n in range(3):
        remote(gr.at[n], gr.at[n], sg.at[n], rg.at[n], dp, mp).wait_recv()
    low = gall[3, :LOW] + gr[0].astype(F32) + gr[1].astype(F32) + gr[2].astype(F32)
    turned = low.T.astype(BF16)
    for b in range(8):
        ys[b] = turned[b * OWN : (b + 1) * OWN]
    y_start(*over_low)
    yr[c, 0] = ys[dp]

    norm_wait(2, NEEDED, ALL)
    rows = nb[2].reshape(32, 128)
    s0, s1 = over_x(rows[:16]), over_z(rows[16:])
    r32 = lax.broadcasted_iota(jnp.int32, (32, 128), 0)
    l32 = lax.broadcasted_iota(jnp.int32, (32, 128), 1)
    x32, z32, j32 = lax.div(r32, 8), lax.rem(lax.div(r32, 2), 4), lax.rem(r32, 2)
    squares = jnp.sum(
        jnp.where(l32 == c * 8 + x32 * 2 + j32, picked(s0, z32, (32, 128)), 0.0)
        + jnp.where(l32 == c * 8 + z32 * 2 + j32, picked(s1, x32, (32, 128)), 0.0),
        axis=1, keepdims=True,
    )
    clip_ref[...] = jnp.sum(
        jnp.where(l32[:, :32] == r32[:, :32], factor(squares), 0.0), axis=0, keepdims=True
    )

    def d_high(k, s):
        gk, ak = place(k)
        aa = mod4(ak + STEPS[s])
        return remote(hs.at[k, lax.div(aa, 2)], hr.at[k, s], shh.at[k, s], rhh.at[k, s], dp, mp_k(k, gk, aa))

    y_wait(*over_high)
    for k in range(2):
        high = yhr[k, 0].astype(F32)
        for dy in range(1, 4):
            high = high + yhr[k, dy].astype(F32)
        for t in range(2):
            hs[k, t] = high[:, t * 128 : (t + 1) * 128].astype(BF16)
        for s in (2, 0, 1):
            d_high(k, s).start()
    total = jnp.dot(hs[0, lax.div(place(0)[1], 2)], eh[0], preferred_element_type=F32)
    total = total + jnp.dot(hs[1, lax.div(place(1)[1], 2)], eh[1], preferred_element_type=F32)
    y_wait(*over_low)
    for k in range(2):
        for dy in range(4):
            total = total + jnp.dot(yr[k, dy], eb[k], preferred_element_type=F32)
    for k in range(2):
        for s in (0, 1, 2):
            remote(hr.at[k, s], hr.at[k, s], shh.at[k, s], rhh.at[k, s], dp, mp).wait_recv()
            total = total + jnp.dot(hr[k, s], eh[k], preferred_element_type=F32)
    grad_ref[...] = total * (1.0 / EXAMPLES)

    d_len.wait_send()
    for k in range(2):
        @pl.when(c != k)
        def _():
            for d in d_own_remote(k):
                d.wait_send()
        for s in range(2):
            for j in range(2):
                d_x(k, s, j).wait_send()
            d_xf(k, s).wait_send()
        for s in range(3):
            for q in range(5):
                d_h(k, s, q).wait_send()
            d_high(k, s).wait_send()
    for q in range(3):
        for n in range(NEEDED if q < 2 else ALL):
            d_norm(q, n).wait_send()
    for n in range(3):
        d_part(n).wait_send()
    for refs in (over_low, over_high):
        for dy in (2, 1, 3):
            for k in range(2):
                d_y(*refs, dy, k).wait_send()
        d_partner(*refs).wait_send()


def exchange(layer_input, output_cot, hidden_cot, hidden_act, lengths):
    dma = pltpu.SemaphoreType.DMA
    hbm = pl.BlockSpec(memory_space=pltpu.HBM)
    vmem = pl.BlockSpec(memory_space=pltpu.VMEM)
    return pl.pallas_call(
        kernel,
        out_shape=(jax.ShapeDtypeStruct((OWN, 2 * ROWS), F32), jax.ShapeDtypeStruct((1, 32), F32)),
        in_specs=[hbm] * 5,
        out_specs=(vmem, vmem),
        scratch_shapes=[
            pltpu.VMEM((2, 4, 2, SLOT, D), BF16),
            pltpu.VMEM((2, 4, 2, 4, ROWS, SLOT), BF16),
            pltpu.VMEM((4, ROWS, D), F32),
            pltpu.VMEM((3, 128, D), BF16),
            pltpu.VMEM((3, 128, D), BF16),
            pltpu.VMEM((256, D), F32),
            pltpu.VMEM((8, OWN, 128), BF16),
            pltpu.VMEM((2, 4, OWN, 128), BF16),
            pltpu.VMEM((8, OWN, 256), BF16),
            pltpu.VMEM((2, 4, OWN, 256), BF16),
            pltpu.VMEM((2, 2, OWN, 128), BF16),
            pltpu.VMEM((2, 3, OWN, 128), BF16),
            pltpu.VMEM((2, 128, 2 * ROWS), BF16),
            pltpu.VMEM((2, 128, 2 * ROWS), BF16),
            pltpu.VMEM((2, 1, 32), jnp.int32),
            pltpu.VMEM((16, 1, SLOT), F32),
            pltpu.VMEM((16, 1, SLOT), F32),
            pltpu.VMEM((16, 1, D), F32),
            pltpu.VMEM((16, 8, 128), F32),
            pltpu.VMEM((3, 32, 1, 128), F32),
            pltpu.VMEM((2, 2, 4, ROWS, D), F32),
            dma((2,)), dma, dma((2, 2, 2)), dma, dma((2, 3, 5)), dma, dma, dma((2, 2)),
            dma((3, 31)), dma((3,)), dma((4, 2)), dma((4, 2)), dma((2, 3)),
            dma((2, 3, 2)), dma, dma((2, 3, 5)), dma, dma, dma((3, 32)), dma((3,)), dma((2, 4)), dma((2, 4)), dma((2, 3)),
            pltpu.SemaphoreType.REGULAR((3,)),
        ],
        compiler_params=pltpu.CompilerParams(has_side_effects=True, collective_id=0, vmem_limit_bytes=56_000_000),
    )(layer_input, output_cot, hidden_cot, hidden_act, lengths)


def local(
    layer_input, output_cot, hidden_act, hidden_cot, lengths, weights, moment_one, moment_two
):
    by_place = (4, 4, 2, ROWS, SLOT)
    gradient, clip = exchange(
        layer_input, output_cot, hidden_cot.reshape(by_place), hidden_act.reshape(by_place), lengths.reshape(1, 32)
    )
    new_moment_one = beta_one * moment_one + (1.0 - beta_one) * gradient
    new_moment_two = beta_two * moment_two + (1.0 - beta_two) * gradient * gradient
    corr_one = 1.0 - beta_one**STEP
    corr_two = 1.0 - beta_two**STEP
    direction = new_moment_one / corr_one / (jnp.sqrt(new_moment_two / corr_two) + adam_eps)
    new_weights = weights - learn_rate * (direction + weight_decay * weights)
    return (new_weights, new_moment_one, new_moment_two, clip.reshape(32))


def solution(mesh):
    return jax.shard_map(
        local,
        mesh=mesh,
        in_specs=(
            P(("dp", "mp"), None, None),
            P(("dp", "mp"), None, None),
            P("dp", "mp", None),
            P("dp", "mp", None),
            P("dp"),
            P("dp", "mp"),
            P("dp", "mp"),
            P("dp", "mp"),
        ),
        out_specs=(P("dp", "mp"), P("dp", "mp"), P("dp", "mp"), P("dp")),
        check_vma=False,
    )
```

```python
import math

import jax
import jax.numpy as jnp
from jax import lax
from jax.experimental import pallas as pl
from jax.experimental.pallas import tpu as pltpu
from jax.sharding import PartitionSpec as P

D = 768
FF = 3072
SLOT = 256
STEP = 10
EXAMPLES = 256
ROWS = 192
OWN = 96

beta_one = 0.9
beta_two = 0.999
adam_eps = 1e-08
learn_rate = 0.001
weight_decay = 0.01
clip_limit = 0.5 * math.sqrt(2.0 * D * FF * SLOT)

MESH = pl.DeviceIdType.MESH
BF16 = jnp.bfloat16
F32 = jnp.float32


def kernel(
    x0_ref, x1_ref, h0_ref, h1_ref, len_ref,
    grad_ref, clip_ref,
    xb, hb, gall, gs, gr, gh, ys, yr, yhs, yhr, hs, hr, eb, eh, lb, mt, ft, fc, npart, nb, p3, xs, hst,
    lsem, llen, sx, sxo, sh, sho, slen, sxf, sn, sg, sy, syh, shh,
    rx, rxo, rh, rho, rlen, rn, rg, ry, ryh, rhh, near,
):
    dp, mp = lax.axis_index("dp"), lax.axis_index("mp")
    c, y = lax.rem(dp, 2), lax.div(dp, 2)
    x, z = lax.div(mp, 4), lax.rem(mp, 4)
    other = 1 - c
    mod4 = lambda v: lax.rem(v + 8, 4)
    g = c * z + (1 - c) * x
    a = c * x + (1 - c) * z
    mp_of = lambda gg, aa: (1 - c) * (gg * 4 + aa) + c * (aa * 4 + gg)

    def remote(src, dst, ssem, rsem, to_dp, to_mp):
        return pltpu.make_async_remote_copy(
            src_ref=src, dst_ref=dst, send_sem=ssem, recv_sem=rsem,
            device_id={"dp": to_dp, "mp": to_mp}, device_id_type=MESH,
        )

    def signal(sem, to_dp, to_mp):
        pl.semaphore_signal(sem, inc=1, device_id={"dp": to_dp, "mp": to_mp}, device_id_type=MESH)

    def loop(count, body):
        lax.fori_loop(0, count, lambda n, carry: (body(n), carry)[1], 0)

    x_refs, h_refs = (x0_ref, x1_ref), (h0_ref, h1_ref)
    STEPS = (1, -1, 2)
    LOW, HIGH = 128, ROWS - 128

    def place(k):
        return (x, z) if k == 0 else (z, x)

    def mp_k(k, gg, aa):
        return gg * 4 + aa if k == 0 else aa * 4 + gg

    def h_slice(k, i, aa):
        return hst.at[k, i, aa] if k == 0 else hst.at[k, aa, i]

    def h_all(k, aa):
        return h_refs[k].at[:, aa] if k == 0 else h_refs[k].at[aa]

    def d_x(k, s, j):
        gk, ak = place(k)
        return remote(xs.at[k, j], xb.at[c, gk, j], sx.at[k, s, j], rx.at[c, s, j],
                      y * 2 + k, mp_k(k, mod4(gk + STEPS[s]), ak))

    def d_h(k, s, q):
        gk, ak = place(k)
        aa = mod4(ak + STEPS[s])
        i = mod4(min(q, 3) - aa)
        src, dst = h_slice(k, i, aa), hb.at[c, i, :, ak]
        if q >= 3:
            src, dst = src.at[q - 3], hb.at[c, i, q - 3, ak]
        return remote(src, dst, sh.at[k, s, q], rh.at[c, s, q], y * 2 + k, mp_k(k, gk, aa))

    def d_own_remote(k):
        gk, ak = place(k)
        return (
            remote(x_refs[k], xb.at[c, gk], sxo, rxo, y * 2 + k, mp),
            remote(h_all(k, ak), hb.at[c, :, :, ak], sho, rho, y * 2 + k, mp),
        )

    def d_own_local(k):
        gk, ak = place(k)
        return (
            pltpu.make_async_copy(x_refs[k], xb.at[c, gk], lsem.at[0]),
            pltpu.make_async_copy(h_all(k, ak), hb.at[c, :, :, ak], lsem.at[1]),
        )

    d_len = remote(len_ref, lb.at[c], slen, rlen, y * 2 + other, mp)
    d_len_local = pltpu.make_async_copy(len_ref, lb.at[c], llen)

    def d_xf(cp, s):
        src = xb.at[cp, mod4(g - STEPS[s]), s]
        return remote(src, src, sxf.at[cp, s], rx.at[cp, 2, s], dp, mp_of(mod4(g + STEPS[s]), a))

    def w_x(cp, s, j):
        ref = xb.at[cp, mod4(g - STEPS[s]), j]
        remote(ref, ref, sx.at[0, s, j], rx.at[cp, s, j], dp, mp).wait_recv()

    def w_xf(cp, s):
        ref = xb.at[cp, mod4(g + 2), s]
        remote(ref, ref, sxf.at[0, s], rx.at[cp, 2, s], dp, mp).wait_recv()

    def w_h(cp, s, q):
        half = slice(None) if q < 3 else q - 3
        ref = hb.at[cp, mod4(min(q, 3) - a), half, mod4(a - STEPS[s])]
        remote(ref, ref, sh.at[0, s, q], rh.at[cp, s, q], dp, mp).wait_recv()

    in_x = [mod4(x + s) * 4 + z for s in STEPS[:2]]
    in_z = [x * 4 + mod4(z + s) for s in STEPS[:2]]
    in_y = [mod4(y + s) * 2 for s in STEPS[:2]]
    staged = [pltpu.make_async_copy(x_refs[k], xs.at[k], lsem.at[2 + k]) for k in range(2)]
    staged_h = [pltpu.make_async_copy(h_refs[k], hst.at[k], lsem.at[4 + k]) for k in range(2)]
    for d in staged + staged_h:
        d.start()
    barrier = pltpu.get_barrier_semaphore()
    signal(barrier, y * 2 + other, mp)
    for k in range(2):
        for to_mp in in_x + in_z:
            signal(barrier, y * 2 + k, to_mp)
        for to_dp in in_y:
            signal(barrier, to_dp + k, mp)
    pl.semaphore_wait(barrier, 13)
    for d in staged:
        d.wait()

    for q in range(2):
        for k in range(2):
            for s in range(2):
                d_x(k, s, q if s == 0 else 1 - q).start()
    d_len_local.start()
    d_len.start()
    for k in range(2):
        @pl.when(c == k)
        def _():
            for d in d_own_local(k):
                d.start()

        @pl.when(c != k)
        def _():
            for d in d_own_remote(k):
                d.start()
    for to_mp in in_x + in_z:
        signal(near.at[0], dp, to_mp)
    for to_dp in in_y:
        signal(near.at[0], to_dp + c, mp)

    f_row = lax.broadcasted_iota(jnp.int32, (128, 2 * ROWS), 0)
    column = lax.broadcasted_iota(jnp.int32, (128, 2 * ROWS), 1)
    for k in range(2):
        eb[k] = jnp.where(column == 2 * f_row + k, 1.0, 0.0).astype(BF16)
        high = f_row - HIGH * lax.rem(place(k)[1], 2)
        hit = jnp.where(column == 2 * (LOW + high) + k, 1.0, 0.0)
        eh[k] = jnp.where(high < HIGH, jnp.where(high >= 0, hit, 0.0), 0.0).astype(BF16)
    npart[...] = jnp.zeros_like(npart)

    d_len_local.wait()
    d_len.wait_recv()
    e_row = lax.broadcasted_iota(jnp.int32, (16, 32), 0)
    e_lane = lax.broadcasted_iota(jnp.int32, (16, 32), 1)
    e_place, e_half = lax.rem(lax.div(e_row, 2), 4), lax.rem(e_row, 2)
    wanted = mp_of(e_place, a) * 2 + e_half
    lens = jnp.where(e_row < 8, lb[0], lb[1]).astype(F32)
    len_col = jnp.sum(jnp.where(e_lane == wanted, lens, 0.0), axis=1, keepdims=True)
    slot = lax.broadcasted_iota(jnp.int32, (16, SLOT), 1).astype(F32)
    mask = jnp.where(slot < len_col, 1.0, 0.0)
    for e in range(16):
        mt[e] = mask[e : e + 1]

    def masked_product(cp, i, j, m):
        h = hb[cp, i, j, m] * mt[cp * 8 + i * 2 + j].astype(BF16)
        return jnp.dot(h, xb[cp, i, j], preferred_element_type=F32)

    def tiles(cp, i, m, halves=(0, 1), keep=False):
        for j in halves:
            e = cp * 8 + i * 2 + j
            p = masked_product(cp, i, j, m)
            if keep:
                p3[cp, j, m] = p
            p = jnp.sum((p * p).reshape(ROWS // 8, 8, D), axis=0)
            part = p[:, :128]
            for n in range(1, D // 128):
                part = part + p[:, n * 128 : (n + 1) * 128]
            npart[e] += part

    for cp in range(2):
        for s in range(2):
            w_x(cp, s, s)
            d_xf(cp, s).start()
    pl.semaphore_wait(near.at[0], 6)
    for d in staged_h:
        d.wait()

    def send_rank(*parts):
        for q in parts:
            for s in (2, 0, 1):
                for k in range(2):
                    d_h(k, s, q).start()

    send_rank(0, 1, 2)
    for to_mp in in_z:
        signal(near.at[1], dp, to_mp)

    for k in range(2):
        @pl.when(c == k)
        def _():
            for d in d_own_local(k):
                d.wait()
    own_x, own_h = xb.at[other, g], hb.at[other, :, :, a]
    remote(own_x, own_x, sxo, rxo, dp, mp).wait_recv()
    remote(own_h, own_h, sho, rho, dp, mp).wait_recv()
    loop(2, lambda cp: tiles(cp, g, a))
    for cp in range(2):
        for s in range(2):
            w_x(cp, s, 1 - s)
    loop(4, lambda n: tiles(lax.div(n, 2), mod4(g + 1 + 2 * lax.rem(n, 2)), a))
    pl.semaphore_wait(near.at[1], 2)
    for to_mp in in_z:
        signal(near.at[2], dp, to_mp)
    for cp in range(2):
        for s in range(2):
            w_xf(cp, s)
    loop(2, lambda cp: tiles(cp, mod4(g + 2), a))
    for cp in range(2):
        for j in range(2):
            p3[cp, j, a] = masked_product(cp, mod4(3 - a), j, a)
    pl.semaphore_wait(near.at[2], 2)

    spot = c * 16 + mp
    r16 = lax.broadcasted_iota(jnp.int32, (16, 128), 0)
    l16 = lax.broadcasted_iota(jnp.int32, (16, 128), 1)
    far_first = sorted(
        [(dx, dz) for dx in range(4) for dz in range(4)],
        key=lambda t: -(min(t[0], 4 - t[0]) + min(t[1], 4 - t[1])),
    )
    same_core = [(2, 0), (1, 0), (3, 0)] + [(dg, da) for da in (2, 1, 3) for dg in range(4)]
    NEEDED, ALL = 19, 31

    def norm_peer(n):
        if n < 16:
            dx, dz = far_first[n]
            return other, mod4(x + dx) * 4 + mod4(z + dz)
        dg, da = same_core[n - 16]
        return c, mp_of(mod4(g + dg), mod4(a + da))

    def d_norm(q, n):
        core, to_mp = norm_peer(n)
        return remote(nb.at[q, spot], nb.at[q, spot], sn.at[q, n], rn.at[q, spot], y * 2 + core, to_mp)

    def norm_send(q):
        col = jnp.sum(jnp.sum(npart[...], axis=1), axis=1, keepdims=True)
        nb[q, spot] = jnp.sum(jnp.where(l16 == r16, col, 0.0), axis=0, keepdims=True)
        for n in range(NEEDED):
            d_norm(q, n).start()

    def picked(table, index, shape):
        out = jnp.zeros(shape, F32)
        for n in range(4):
            out = out + jnp.where(index == n, table[n : n + 1], 0.0)
        return out

    def factor(squares):
        return clip_limit / jnp.maximum(jnp.sqrt(squares), clip_limit)

    def norm_wait(q, first, last):
        for n in range(first, last):
            core, from_mp = norm_peer(n)
            ref = nb.at[q, core * 16 + from_mp]
            remote(ref, ref, sn.at[q, n], rn.at[q, core * 16 + from_mp], dp, mp).wait_recv()

    def over_x(rows):
        return rows[0:4] + rows[4:8] + rows[8:12] + rows[12:16]

    def over_z(rows):
        return jnp.concatenate(
            [jnp.sum(rows[4 * n : 4 * n + 4], axis=0, keepdims=True) for n in range(4)], axis=0
        )

    def norm_take(q):
        norm_wait(q, 0, NEEDED)
        rows = nb[q, pl.ds(other * 16, 16)].reshape(16, 128)
        others = jnp.where(c == 0, over_z(rows), over_x(rows))
        mine = nb[q, c * 16 + mp_of(0, a)]
        for n in range(1, 4):
            mine = mine + nb[q, c * 16 + mp_of(n, a)]
        place16, half16 = lax.rem(lax.div(r16, 2), 4), lax.rem(r16, 2)
        squares = jnp.sum(
            jnp.where(l16 == r16, mine, 0.0)
            + jnp.where(l16 == lax.div(r16, 8) * 8 + a * 2 + half16, picked(others, place16, (16, 128)), 0.0),
            axis=1, keepdims=True,
        )
        scale = factor(squares)
        if q == 2:
            for e in range(16):
                fc[e] = jnp.broadcast_to(scale[e : e + 1], (1, D))
        else:
            scaled_mask = mask * scale
            for e in range(16):
                ft[e] = scaled_mask[e : e + 1]

    def owner(n):
        return mod4(a + 2 - n + 3 * (n // 2) - 2 * (n // 3))

    def products(m, ranks):
        total = None
        for r in ranks:
            for cp in range(2):
                for j in range(2):
                    i = mod4(r - a)
                    h = (hb[cp, i, j, m].astype(F32) * ft[cp * 8 + i * 2 + j]).astype(BF16)
                    p = jnp.dot(h, xb[cp, i, j], preferred_element_type=F32)
                    total = p if total is None else total + p
        return total

    def early(n):
        gall[n] = products(owner(n), (0, 1))

    def third(n):
        gall[n] += products(owner(n), (2,))

    for q in range(5):
        for s in (2, 0, 1):
            for cp in range(2):
                w_h(cp, s, q)
            if q < 3:
                loop(2, lambda cp: tiles(cp, mod4(q - a), mod4(a - STEPS[s])))
            else:
                for cp in range(2):
                    tiles(cp, mod4(3 - a), mod4(a - STEPS[s]), (q - 3,), True)
        if q in (1, 2):
            norm_send(q - 1)
        if q == 1:
            send_rank(3, 4)
        if q == 2:
            norm_take(0)
            loop(4, early)
    norm_send(2)
    norm_take(1)
    loop(4, third)
    norm_take(2)

    def d_part(n):
        return remote(gs.at[n], gr.at[n], sg.at[n], rg.at[n], dp, mp_of(g, owner(n)))

    def final_rows(n, row):
        rows = pl.ds(row, 16)
        total = gall[n, rows]
        for cp in range(2):
            for j in range(2):
                total = total + fc[cp * 8 + mod4(3 - a) * 2 + j] * p3[cp, j, owner(n), rows]
        return total

    for n in range(4):
        for row in range(0, LOW, 16):
            if n < 3:
                gs[n, row : row + 16] = final_rows(n, row).astype(BF16)
            else:
                gall[n, row : row + 16] = final_rows(n, row)
        if n < 3:
            d_part(n).start()
        for row in range(LOW, ROWS, 16):
            gh[pl.ds(pl.multiple_of(owner(n) * HIGH + row - LOW, 16), 16)] = final_rows(n, row)

    def d_y(src, dst, ssem, rsem, dy, k):
        to_dp = mod4(y + dy) * 2 + k
        return remote(src.at[to_dp], dst.at[c, dy], ssem.at[dy, k], rsem.at[c, dy], to_dp, mp)

    def d_partner(src, dst, ssem, rsem):
        to_dp = y * 2 + other
        return remote(src.at[to_dp], dst.at[c, 0], ssem.at[0, 0], rsem.at[c, 0], to_dp, mp)

    def y_start(*refs):
        for dy in (2, 1, 3):
            for k in range(2):
                d_y(*refs, dy, k).start()
        d_partner(*refs).start()

    def y_wait(src, dst, ssem, rsem):
        ref = dst.at[other, 0]
        remote(ref, ref, ssem.at[0, 1], rsem.at[other, 0], dp, mp).wait_recv()
        for dy in (1, 3, 2):
            for k in range(2):
                ref = dst.at[k, dy]
                remote(ref, ref, ssem.at[dy, k], rsem.at[k, dy], dp, mp).wait_recv()

    over_low, over_high = (ys, yr, sy, ry), (yhs, yhr, syh, ryh)
    for n in range(NEEDED, ALL):
        d_norm(2, n).start()
    turned = gh[...].T.astype(BF16)
    for b in range(8):
        yhs[b] = turned[b * OWN : (b + 1) * OWN]
    y_start(*over_high)
    yhr[c, 0] = yhs[dp]

    d_len.wait_send()
    for k in range(2):
        @pl.when(c != k)
        def _():
            for d in d_own_remote(k):
                d.wait_send()
        for s in range(2):
            for j in range(2):
                d_x(k, s, j).wait_send()
            d_xf(k, s).wait_send()
        for s in range(3):
            for q in range(5):
                d_h(k, s, q).wait_send()
    for q in range(3):
        for n in range(NEEDED):
            d_norm(q, n).wait_send()

    for n in range(3):
        remote(gr.at[n], gr.at[n], sg.at[n], rg.at[n], dp, mp).wait_recv()
    low = gall[3, :LOW] + gr[0].astype(F32) + gr[1].astype(F32) + gr[2].astype(F32)
    turned = low.T.astype(BF16)
    for b in range(8):
        ys[b] = turned[b * OWN : (b + 1) * OWN]
    y_start(*over_low)
    yr[c, 0] = ys[dp]

    def d_high(k, s):
        gk, ak = place(k)
        aa = mod4(ak + STEPS[s])
        return remote(hs.at[k, lax.div(aa, 2)], hr.at[k, s], shh.at[k, s], rhh.at[k, s], dp, mp_k(k, gk, aa))

    y_wait(*over_high)
    for k in range(2):
        high = yhr[k, 0].astype(F32)
        for dy in range(1, 4):
            high = high + yhr[k, dy].astype(F32)
        for t in range(2):
            hs[k, t] = high[:, t * 128 : (t + 1) * 128].astype(BF16)
        for s in (2, 0, 1):
            d_high(k, s).start()
    norm_wait(2, NEEDED, ALL)
    rows = nb[2].reshape(32, 128)
    s0, s1 = over_x(rows[:16]), over_z(rows[16:])
    r32 = lax.broadcasted_iota(jnp.int32, (32, 128), 0)
    l32 = lax.broadcasted_iota(jnp.int32, (32, 128), 1)
    x32, z32, j32 = lax.div(r32, 8), lax.rem(lax.div(r32, 2), 4), lax.rem(r32, 2)
    squares = jnp.sum(
        jnp.where(l32 == c * 8 + x32 * 2 + j32, picked(s0, z32, (32, 128)), 0.0)
        + jnp.where(l32 == c * 8 + z32 * 2 + j32, picked(s1, x32, (32, 128)), 0.0),
        axis=1, keepdims=True,
    )
    clip_ref[...] = jnp.sum(
        jnp.where(l32[:, :32] == r32[:, :32], factor(squares), 0.0), axis=0, keepdims=True
    )
    for n in range(NEEDED, ALL):
        d_norm(2, n).wait_send()
    for n in range(3):
        d_part(n).wait_send()

    total = jnp.dot(hs[0, lax.div(place(0)[1], 2)], eh[0], preferred_element_type=F32)
    total = total + jnp.dot(hs[1, lax.div(place(1)[1], 2)], eh[1], preferred_element_type=F32)
    y_wait(*over_low)
    for k in range(2):
        for dy in range(4):
            total = total + jnp.dot(yr[k, dy], eb[k], preferred_element_type=F32)
    for k in range(2):
        for s in (0, 1, 2):
            remote(hr.at[k, s], hr.at[k, s], shh.at[k, s], rhh.at[k, s], dp, mp).wait_recv()
            total = total + jnp.dot(hr[k, s], eh[k], preferred_element_type=F32)
    grad_ref[...] = total * (1.0 / EXAMPLES)

    for k in range(2):
        for s in range(3):
            d_high(k, s).wait_send()
    for refs in (over_low, over_high):
        for dy in (2, 1, 3):
            for k in range(2):
                d_y(*refs, dy, k).wait_send()
        d_partner(*refs).wait_send()

def exchange(layer_input, output_cot, hidden_cot, hidden_act, lengths):
    dma = pltpu.SemaphoreType.DMA
    hbm = pl.BlockSpec(memory_space=pltpu.HBM)
    vmem = pl.BlockSpec(memory_space=pltpu.VMEM)
    return pl.pallas_call(
        kernel,
        out_shape=(jax.ShapeDtypeStruct((OWN, 2 * ROWS), F32), jax.ShapeDtypeStruct((1, 32), F32)),
        in_specs=[hbm] * 5,
        out_specs=(vmem, vmem),
        scratch_shapes=[
            pltpu.VMEM((2, 4, 2, SLOT, D), BF16),
            pltpu.VMEM((2, 4, 2, 4, ROWS, SLOT), BF16),
            pltpu.VMEM((4, ROWS, D), F32),
            pltpu.VMEM((3, 128, D), BF16),
            pltpu.VMEM((3, 128, D), BF16),
            pltpu.VMEM((256, D), F32),
            pltpu.VMEM((8, OWN, 128), BF16),
            pltpu.VMEM((2, 4, OWN, 128), BF16),
            pltpu.VMEM((8, OWN, 256), BF16),
            pltpu.VMEM((2, 4, OWN, 256), BF16),
            pltpu.VMEM((2, 2, OWN, 128), BF16),
            pltpu.VMEM((2, 3, OWN, 128), BF16),
            pltpu.VMEM((2, 128, 2 * ROWS), BF16),
            pltpu.VMEM((2, 128, 2 * ROWS), BF16),
            pltpu.VMEM((2, 1, 32), jnp.int32),
            pltpu.VMEM((16, 1, SLOT), F32),
            pltpu.VMEM((16, 1, SLOT), F32),
            pltpu.VMEM((16, 1, D), F32),
            pltpu.VMEM((16, 8, 128), F32),
            pltpu.VMEM((3, 32, 1, 128), F32),
            pltpu.VMEM((2, 2, 4, ROWS, D), F32),
            pltpu.VMEM((2, 2, SLOT, D), BF16),
            pltpu.VMEM((2, 4, 4, 2, ROWS, SLOT), BF16),
            dma((6,)), dma, dma((2, 2, 2)), dma, dma((2, 3, 5)), dma, dma, dma((2, 2)),
            dma((3, 31)), dma((3,)), dma((4, 2)), dma((4, 2)), dma((2, 3)),
            dma((2, 3, 2)), dma, dma((2, 3, 5)), dma, dma, dma((3, 32)), dma((3,)), dma((2, 4)), dma((2, 4)), dma((2, 3)),
            pltpu.SemaphoreType.REGULAR((3,)),
        ],
        compiler_params=pltpu.CompilerParams(has_side_effects=True, collective_id=0, vmem_limit_bytes=56_000_000),
    )(layer_input, output_cot, hidden_cot, hidden_act, lengths)


def local(
    layer_input, output_cot, hidden_act, hidden_cot, lengths, weights, moment_one, moment_two
):
    by_place = (4, 4, 2, ROWS, SLOT)
    gradient, clip = exchange(
        layer_input, output_cot, hidden_cot.reshape(by_place), hidden_act.reshape(by_place), lengths.reshape(1, 32)
    )
    new_moment_one = beta_one * moment_one + (1.0 - beta_one) * gradient
    new_moment_two = beta_two * moment_two + (1.0 - beta_two) * gradient * gradient
    corr_one = 1.0 - beta_one**STEP
    corr_two = 1.0 - beta_two**STEP
    direction = new_moment_one / corr_one / (jnp.sqrt(new_moment_two / corr_two) + adam_eps)
    new_weights = weights - learn_rate * (direction + weight_decay * weights)
    return (new_weights, new_moment_one, new_moment_two, clip.reshape(32))


def solution(mesh):
    return jax.shard_map(
        local,
        mesh=mesh,
        in_specs=(
            P(("dp", "mp"), None, None),
            P(("dp", "mp"), None, None),
            P("dp", "mp", None),
            P("dp", "mp", None),
            P("dp"),
            P("dp", "mp"),
            P("dp", "mp"),
            P("dp", "mp"),
        ),
        out_specs=(P("dp", "mp"), P("dp", "mp"), P("dp", "mp"), P("dp")),
        check_vma=False,
    )
```

```python
import math

import jax
import jax.numpy as jnp
from jax import lax
from jax.experimental import pallas as pl
from jax.experimental.pallas import tpu as pltpu
from jax.sharding import PartitionSpec as P

D = 768
FF = 3072
SLOT = 256
STEP = 10
EXAMPLES = 256
ROWS = 192
OWN = 96

beta_one = 0.9
beta_two = 0.999
adam_eps = 1e-08
learn_rate = 0.001
weight_decay = 0.01
clip_limit = 0.5 * math.sqrt(2.0 * D * FF * SLOT)

MESH = pl.DeviceIdType.MESH
BF16 = jnp.bfloat16
F32 = jnp.float32


def kernel(
    x0_ref, x1_ref, h0_ref, h1_ref, len_ref,
    grad_ref, clip_ref,
    xb, hb, gall, gs, gr, gh, ys, yr, yhs, yhr, hs, hr, eb, eh, lb, mt, ft, fc, npart, nb, p3, xs, hst,
    lsem, llen, sx, sxo, sh, sho, slen, sxf, sn, sg, sy, syh, shh,
    rx, rxo, rh, rho, rlen, rn, rg, ry, ryh, rhh, near,
):
    dp, mp = lax.axis_index("dp"), lax.axis_index("mp")
    c, y = lax.rem(dp, 2), lax.div(dp, 2)
    x, z = lax.div(mp, 4), lax.rem(mp, 4)
    other = 1 - c
    mod4 = lambda v: lax.rem(v + 8, 4)
    g = c * z + (1 - c) * x
    a = c * x + (1 - c) * z
    mp_of = lambda gg, aa: (1 - c) * (gg * 4 + aa) + c * (aa * 4 + gg)

    def remote(src, dst, ssem, rsem, to_dp, to_mp):
        return pltpu.make_async_remote_copy(
            src_ref=src, dst_ref=dst, send_sem=ssem, recv_sem=rsem,
            device_id={"dp": to_dp, "mp": to_mp}, device_id_type=MESH,
        )

    def signal(sem, to_dp, to_mp):
        pl.semaphore_signal(sem, inc=1, device_id={"dp": to_dp, "mp": to_mp}, device_id_type=MESH)

    def loop(count, body):
        lax.fori_loop(0, count, lambda n, carry: (body(n), carry)[1], 0)

    x_refs, h_refs = (x0_ref, x1_ref), (h0_ref, h1_ref)
    STEPS = (1, -1, 2)
    LOW, HIGH = 128, ROWS - 128

    def place(k):
        return (x, z) if k == 0 else (z, x)

    def mp_k(k, gg, aa):
        return gg * 4 + aa if k == 0 else aa * 4 + gg

    def h_slice(k, i, aa):
        return hst.at[k, i, aa] if k == 0 else hst.at[k, aa, i]

    def h_all(k, aa):
        return h_refs[k].at[:, aa] if k == 0 else h_refs[k].at[aa]

    def d_x(k, s, j):
        gk, ak = place(k)
        return remote(xs.at[k, j], xb.at[c, gk, j], sx.at[k, s, j], rx.at[c, s, j],
                      y * 2 + k, mp_k(k, mod4(gk + STEPS[s]), ak))

    def d_h(k, s, q):
        gk, ak = place(k)
        aa = mod4(ak + STEPS[s])
        i = mod4(min(q, 3) - aa)
        src, dst = h_slice(k, i, aa), hb.at[c, i, :, ak]
        if q >= 3:
            src, dst = src.at[q - 3], hb.at[c, i, q - 3, ak]
        return remote(src, dst, sh.at[k, s, q], rh.at[c, s, q], y * 2 + k, mp_k(k, gk, aa))

    def d_own_remote(k):
        gk, ak = place(k)
        return (
            remote(x_refs[k], xb.at[c, gk], sxo, rxo, y * 2 + k, mp),
            remote(h_all(k, ak), hb.at[c, :, :, ak], sho, rho, y * 2 + k, mp),
        )

    def d_own_local(k):
        gk, ak = place(k)
        return (
            pltpu.make_async_copy(x_refs[k], xb.at[c, gk], lsem.at[0]),
            pltpu.make_async_copy(h_all(k, ak), hb.at[c, :, :, ak], lsem.at[1]),
        )

    d_len = remote(len_ref, lb.at[c], slen, rlen, y * 2 + other, mp)
    d_len_local = pltpu.make_async_copy(len_ref, lb.at[c], llen)

    def d_xf(cp, s):
        src = xb.at[cp, mod4(g - STEPS[s]), s]
        return remote(src, src, sxf.at[cp, s], rx.at[cp, 2, s], dp, mp_of(mod4(g + STEPS[s]), a))

    def w_x(cp, s, j):
        ref = xb.at[cp, mod4(g - STEPS[s]), j]
        remote(ref, ref, sx.at[0, s, j], rx.at[cp, s, j], dp, mp).wait_recv()

    def w_xf(cp, s):
        ref = xb.at[cp, mod4(g + 2), s]
        remote(ref, ref, sxf.at[0, s], rx.at[cp, 2, s], dp, mp).wait_recv()

    def w_h(cp, s, q):
        half = slice(None) if q < 3 else q - 3
        ref = hb.at[cp, mod4(min(q, 3) - a), half, mod4(a - STEPS[s])]
        remote(ref, ref, sh.at[0, s, q], rh.at[cp, s, q], dp, mp).wait_recv()

    in_x = [mod4(x + s) * 4 + z for s in STEPS[:2]]
    in_z = [x * 4 + mod4(z + s) for s in STEPS[:2]]
    in_y = [mod4(y + s) * 2 for s in STEPS[:2]]
    staged = [pltpu.make_async_copy(x_refs[k], xs.at[k], lsem.at[2 + k]) for k in range(2)]
    staged_h = [pltpu.make_async_copy(h_refs[k], hst.at[k], lsem.at[4 + k]) for k in range(2)]
    for d in staged + staged_h:
        d.start()
    barrier = pltpu.get_barrier_semaphore()
    signal(barrier, y * 2 + other, mp)
    for k in range(2):
        for to_mp in in_x + in_z:
            signal(barrier, y * 2 + k, to_mp)
        for to_dp in in_y:
            signal(barrier, to_dp + k, mp)
    pl.semaphore_wait(barrier, 13)
    for d in staged:
        d.wait()

    for q in range(2):
        for k in range(2):
            for s in range(2):
                d_x(k, s, q if s == 0 else 1 - q).start()
    d_len_local.start()
    d_len.start()
    for k in range(2):
        @pl.when(c == k)
        def _():
            for d in d_own_local(k):
                d.start()

        @pl.when(c != k)
        def _():
            for d in d_own_remote(k):
                d.start()
    for to_mp in in_x + in_z:
        signal(near.at[0], dp, to_mp)
    for to_dp in in_y:
        signal(near.at[0], to_dp + c, mp)

    f_row = lax.broadcasted_iota(jnp.int32, (128, 2 * ROWS), 0)
    column = lax.broadcasted_iota(jnp.int32, (128, 2 * ROWS), 1)
    for k in range(2):
        eb[k] = jnp.where(column == 2 * f_row + k, 1.0, 0.0).astype(BF16)
        high = f_row - HIGH * lax.rem(place(k)[1], 2)
        hit = jnp.where(column == 2 * (LOW + high) + k, 1.0, 0.0)
        eh[k] = jnp.where(high < HIGH, jnp.where(high >= 0, hit, 0.0), 0.0).astype(BF16)
    npart[...] = jnp.zeros_like(npart)

    d_len_local.wait()
    d_len.wait_recv()
    e_row = lax.broadcasted_iota(jnp.int32, (16, 32), 0)
    e_lane = lax.broadcasted_iota(jnp.int32, (16, 32), 1)
    e_place, e_half = lax.rem(lax.div(e_row, 2), 4), lax.rem(e_row, 2)
    wanted = mp_of(e_place, a) * 2 + e_half
    lens = jnp.where(e_row < 8, lb[0], lb[1]).astype(F32)
    len_col = jnp.sum(jnp.where(e_lane == wanted, lens, 0.0), axis=1, keepdims=True)
    slot = lax.broadcasted_iota(jnp.int32, (16, SLOT), 1).astype(F32)
    mask = jnp.where(slot < len_col, 1.0, 0.0)
    for e in range(16):
        mt[e] = mask[e : e + 1]

    def masked_product(cp, i, j, m):
        h = hb[cp, i, j, m] * mt[cp * 8 + i * 2 + j].astype(BF16)
        return jnp.dot(h, xb[cp, i, j], preferred_element_type=F32)

    def tiles(cp, i, m, halves=(0, 1), keep=False):
        for j in halves:
            e = cp * 8 + i * 2 + j
            p = masked_product(cp, i, j, m)
            if keep:
                p3[cp, j, m] = p
            p = jnp.sum((p * p).reshape(ROWS // 8, 8, D), axis=0)
            part = p[:, :128]
            for n in range(1, D // 128):
                part = part + p[:, n * 128 : (n + 1) * 128]
            npart[e] += part

    for cp in range(2):
        for s in range(2):
            w_x(cp, s, s)
            d_xf(cp, s).start()
    pl.semaphore_wait(near.at[0], 6)
    for d in staged_h:
        d.wait()

    def send_rank(*parts):
        for q in parts:
            for s in (2, 0, 1):
                for k in range(2):
                    d_h(k, s, q).start()

    send_rank(0, 1, 2)
    for to_mp in in_z:
        signal(near.at[1], dp, to_mp)

    for k in range(2):
        @pl.when(c == k)
        def _():
            for d in d_own_local(k):
                d.wait()
    own_x, own_h = xb.at[other, g], hb.at[other, :, :, a]
    remote(own_x, own_x, sxo, rxo, dp, mp).wait_recv()
    remote(own_h, own_h, sho, rho, dp, mp).wait_recv()
    loop(2, lambda cp: tiles(cp, g, a))
    for cp in range(2):
        for s in range(2):
            w_x(cp, s, 1 - s)
    loop(4, lambda n: tiles(lax.div(n, 2), mod4(g + 1 + 2 * lax.rem(n, 2)), a))
    pl.semaphore_wait(near.at[1], 2)
    for to_mp in in_z:
        signal(near.at[2], dp, to_mp)
    for cp in range(2):
        for s in range(2):
            w_xf(cp, s)
    loop(2, lambda cp: tiles(cp, mod4(g + 2), a))
    for cp in range(2):
        for j in range(2):
            p3[cp, j, a] = masked_product(cp, mod4(3 - a), j, a)
    pl.semaphore_wait(near.at[2], 2)

    spot = c * 16 + mp
    r16 = lax.broadcasted_iota(jnp.int32, (16, 128), 0)
    l16 = lax.broadcasted_iota(jnp.int32, (16, 128), 1)
    far_first = sorted(
        [(dx, dz) for dx in range(4) for dz in range(4)],
        key=lambda t: -(min(t[0], 4 - t[0]) + min(t[1], 4 - t[1])),
    )
    same_core = [(2, 0), (1, 0), (3, 0)] + [(dg, da) for da in (2, 1, 3) for dg in range(4)]
    NEEDED, ALL = 19, 31

    def norm_peer(n):
        if n < 16:
            dx, dz = far_first[n]
            return other, mod4(x + dx) * 4 + mod4(z + dz)
        dg, da = same_core[n - 16]
        return c, mp_of(mod4(g + dg), mod4(a + da))

    def d_norm(q, n):
        core, to_mp = norm_peer(n)
        return remote(nb.at[q, spot], nb.at[q, spot], sn.at[q, n], rn.at[q, spot], y * 2 + core, to_mp)

    def norm_send(q):
        col = jnp.sum(jnp.sum(npart[...], axis=1), axis=1, keepdims=True)
        nb[q, spot] = jnp.sum(jnp.where(l16 == r16, col, 0.0), axis=0, keepdims=True)
        for n in range(NEEDED):
            d_norm(q, n).start()

    def picked(table, index, shape):
        out = jnp.zeros(shape, F32)
        for n in range(4):
            out = out + jnp.where(index == n, table[n : n + 1], 0.0)
        return out

    def factor(squares):
        return clip_limit / jnp.maximum(jnp.sqrt(squares), clip_limit)

    def norm_wait(q, first, last):
        for n in range(first, last):
            core, from_mp = norm_peer(n)
            ref = nb.at[q, core * 16 + from_mp]
            remote(ref, ref, sn.at[q, n], rn.at[q, core * 16 + from_mp], dp, mp).wait_recv()

    def over_x(rows):
        return rows[0:4] + rows[4:8] + rows[8:12] + rows[12:16]

    def over_z(rows):
        return jnp.concatenate(
            [jnp.sum(rows[4 * n : 4 * n + 4], axis=0, keepdims=True) for n in range(4)], axis=0
        )

    def norm_take(q):
        norm_wait(q, 0, NEEDED)
        rows = nb[q, pl.ds(other * 16, 16)].reshape(16, 128)
        others = jnp.where(c == 0, over_z(rows), over_x(rows))
        mine = nb[q, c * 16 + mp_of(0, a)]
        for n in range(1, 4):
            mine = mine + nb[q, c * 16 + mp_of(n, a)]
        place16, half16 = lax.rem(lax.div(r16, 2), 4), lax.rem(r16, 2)
        squares = jnp.sum(
            jnp.where(l16 == r16, mine, 0.0)
            + jnp.where(l16 == lax.div(r16, 8) * 8 + a * 2 + half16, picked(others, place16, (16, 128)), 0.0),
            axis=1, keepdims=True,
        )
        scale = factor(squares)
        if q == 2:
            for e in range(16):
                fc[e] = jnp.broadcast_to(scale[e : e + 1], (1, D))
        else:
            scaled_mask = mask * scale
            for e in range(16):
                ft[e] = scaled_mask[e : e + 1]

    def owner(n):
        return mod4(a + 2 - n + 3 * (n // 2) - 2 * (n // 3))

    def products(m, ranks):
        total = None
        for r in ranks:
            for cp in range(2):
                for j in range(2):
                    i = mod4(r - a)
                    h = (hb[cp, i, j, m].astype(F32) * ft[cp * 8 + i * 2 + j]).astype(BF16)
                    p = jnp.dot(h, xb[cp, i, j], preferred_element_type=F32)
                    total = p if total is None else total + p
        return total

    def early(n):
        gall[n] = products(owner(n), (0, 1))

    def third(n):
        gall[n] += products(owner(n), (2,))

    for q in range(5):
        for s in (2, 0, 1):
            for cp in range(2):
                w_h(cp, s, q)
            if q < 3:
                loop(2, lambda cp: tiles(cp, mod4(q - a), mod4(a - STEPS[s])))
            else:
                for cp in range(2):
                    tiles(cp, mod4(3 - a), mod4(a - STEPS[s]), (q - 3,), True)
        if q in (1, 2):
            norm_send(q - 1)
        if q == 1:
            send_rank(3, 4)
        if q == 2:
            norm_take(0)
            loop(4, early)
    norm_send(2)
    norm_take(1)
    loop(4, third)
    norm_take(2)

    def d_part(n):
        return remote(gs.at[n], gr.at[n], sg.at[n], rg.at[n], dp, mp_of(g, owner(n)))

    def final_rows(n, row):
        rows = pl.ds(row, 16)
        total = gall[n, rows]
        for cp in range(2):
            for j in range(2):
                total = total + fc[cp * 8 + mod4(3 - a) * 2 + j] * p3[cp, j, owner(n), rows]
        return total

    for n in range(4):
        for row in range(0, LOW, 16):
            if n < 3:
                gs[n, row : row + 16] = final_rows(n, row).astype(BF16)
            else:
                gall[n, row : row + 16] = final_rows(n, row)
        if n < 3:
            d_part(n).start()
        for row in range(LOW, ROWS, 16):
            gh[pl.ds(pl.multiple_of(owner(n) * HIGH + row - LOW, 16), 16)] = final_rows(n, row)

    def d_y(src, dst, ssem, rsem, dy, k):
        to_dp = mod4(y + dy) * 2 + k
        return remote(src.at[to_dp], dst.at[c, dy], ssem.at[dy, k], rsem.at[c, dy], to_dp, mp)

    def d_partner(src, dst, ssem, rsem):
        to_dp = y * 2 + other
        return remote(src.at[to_dp], dst.at[c, 0], ssem.at[0, 0], rsem.at[c, 0], to_dp, mp)

    def y_start(*refs):
        for dy in (2, 1, 3):
            for k in range(2):
                d_y(*refs, dy, k).start()
        d_partner(*refs).start()

    def y_wait(src, dst, ssem, rsem):
        ref = dst.at[other, 0]
        remote(ref, ref, ssem.at[0, 1], rsem.at[other, 0], dp, mp).wait_recv()
        for dy in (1, 3, 2):
            for k in range(2):
                ref = dst.at[k, dy]
                remote(ref, ref, ssem.at[dy, k], rsem.at[k, dy], dp, mp).wait_recv()

    over_low, over_high = (ys, yr, sy, ry), (yhs, yhr, syh, ryh)
    for n in range(NEEDED, ALL):
        d_norm(2, n).start()
    turned = gh[...].T.astype(BF16)
    for b in range(8):
        yhs[b] = turned[b * OWN : (b + 1) * OWN]
    y_start(*over_high)
    yhr[c, 0] = yhs[dp]

    d_len.wait_send()
    for k in range(2):
        @pl.when(c != k)
        def _():
            for d in d_own_remote(k):
                d.wait_send()
        for s in range(2):
            for j in range(2):
                d_x(k, s, j).wait_send()
            d_xf(k, s).wait_send()
        for s in range(3):
            for q in range(5):
                d_h(k, s, q).wait_send()
    for q in range(3):
        for n in range(NEEDED):
            d_norm(q, n).wait_send()

    for n in range(3):
        remote(gr.at[n], gr.at[n], sg.at[n], rg.at[n], dp, mp).wait_recv()
    low = gall[3, :LOW] + gr[0].astype(F32) + gr[1].astype(F32) + gr[2].astype(F32)
    turned = low.T.astype(BF16)
    for b in range(8):
        ys[b] = turned[b * OWN : (b + 1) * OWN]
    y_start(*over_low)
    yr[c, 0] = ys[dp]

    def d_high(k, s):
        gk, ak = place(k)
        aa = mod4(ak + STEPS[s])
        return remote(hs.at[k, lax.div(aa, 2)], hr.at[k, s], shh.at[k, s], rhh.at[k, s], dp, mp_k(k, gk, aa))

    y_wait(*over_high)
    for k in range(2):
        high = yhr[k, 0].astype(F32)
        for dy in range(1, 4):
            high = high + yhr[k, dy].astype(F32)
        for t in range(2):
            hs[k, t] = high[:, t * 128 : (t + 1) * 128].astype(BF16)
        for s in (2, 0, 1):
            d_high(k, s).start()
    norm_wait(2, NEEDED, ALL)
    rows = nb[2].reshape(32, 128)
    s0, s1 = over_x(rows[:16]), over_z(rows[16:])
    r32 = lax.broadcasted_iota(jnp.int32, (32, 128), 0)
    l32 = lax.broadcasted_iota(jnp.int32, (32, 128), 1)
    x32, z32, j32 = lax.div(r32, 8), lax.rem(lax.div(r32, 2), 4), lax.rem(r32, 2)
    squares = jnp.sum(
        jnp.where(l32 == c * 8 + x32 * 2 + j32, picked(s0, z32, (32, 128)), 0.0)
        + jnp.where(l32 == c * 8 + z32 * 2 + j32, picked(s1, x32, (32, 128)), 0.0),
        axis=1, keepdims=True,
    )
    clip_ref[...] = jnp.sum(
        jnp.where(l32[:, :32] == r32[:, :32], factor(squares), 0.0), axis=0, keepdims=True
    )
    for n in range(NEEDED, ALL):
        d_norm(2, n).wait_send()
    for n in range(3):
        d_part(n).wait_send()

    total = jnp.dot(hs[0, lax.div(place(0)[1], 2)], eh[0], preferred_element_type=F32)
    total = total + jnp.dot(hs[1, lax.div(place(1)[1], 2)], eh[1], preferred_element_type=F32)
    def spread(blocks, count, table):
        out = jnp.dot(blocks.reshape(count * OWN, 128), table, preferred_element_type=F32)
        return sum(out[n * OWN : (n + 1) * OWN] for n in range(1, count)) + out[:OWN]

    y_wait(*over_low)
    for k in range(2):
        total = total + spread(yr[k], 4, eb[k])
    for k in range(2):
        for s in (0, 1, 2):
            remote(hr.at[k, s], hr.at[k, s], shh.at[k, s], rhh.at[k, s], dp, mp).wait_recv()
    for k in range(2):
        total = total + spread(hr[k], 3, eh[k])
    grad_ref[...] = total * (1.0 / EXAMPLES)

    for k in range(2):
        for s in range(3):
            d_high(k, s).wait_send()
    for refs in (over_low, over_high):
        for dy in (2, 1, 3):
            for k in range(2):
                d_y(*refs, dy, k).wait_send()
        d_partner(*refs).wait_send()

def exchange(layer_input, output_cot, hidden_cot, hidden_act, lengths):
    dma = pltpu.SemaphoreType.DMA
    hbm = pl.BlockSpec(memory_space=pltpu.HBM)
    vmem = pl.BlockSpec(memory_space=pltpu.VMEM)
    return pl.pallas_call(
        kernel,
        out_shape=(jax.ShapeDtypeStruct((OWN, 2 * ROWS), F32), jax.ShapeDtypeStruct((1, 32), F32)),
        in_specs=[hbm] * 5,
        out_specs=(vmem, vmem),
        scratch_shapes=[
            pltpu.VMEM((2, 4, 2, SLOT, D), BF16),
            pltpu.VMEM((2, 4, 2, 4, ROWS, SLOT), BF16),
            pltpu.VMEM((4, ROWS, D), F32),
            pltpu.VMEM((3, 128, D), BF16),
            pltpu.VMEM((3, 128, D), BF16),
            pltpu.VMEM((256, D), F32),
            pltpu.VMEM((8, OWN, 128), BF16),
            pltpu.VMEM((2, 4, OWN, 128), BF16),
            pltpu.VMEM((8, OWN, 256), BF16),
            pltpu.VMEM((2, 4, OWN, 256), BF16),
            pltpu.VMEM((2, 2, OWN, 128), BF16),
            pltpu.VMEM((2, 3, OWN, 128), BF16),
            pltpu.VMEM((2, 128, 2 * ROWS), BF16),
            pltpu.VMEM((2, 128, 2 * ROWS), BF16),
            pltpu.VMEM((2, 1, 32), jnp.int32),
            pltpu.VMEM((16, 1, SLOT), F32),
            pltpu.VMEM((16, 1, SLOT), F32),
            pltpu.VMEM((16, 1, D), F32),
            pltpu.VMEM((16, 8, 128), F32),
            pltpu.VMEM((3, 32, 1, 128), F32),
            pltpu.VMEM((2, 2, 4, ROWS, D), F32),
            pltpu.VMEM((2, 2, SLOT, D), BF16),
            pltpu.VMEM((2, 4, 4, 2, ROWS, SLOT), BF16),
            dma((6,)), dma, dma((2, 2, 2)), dma, dma((2, 3, 5)), dma, dma, dma((2, 2)),
            dma((3, 31)), dma((3,)), dma((4, 2)), dma((4, 2)), dma((2, 3)),
            dma((2, 3, 2)), dma, dma((2, 3, 5)), dma, dma, dma((3, 32)), dma((3,)), dma((2, 4)), dma((2, 4)), dma((2, 3)),
            pltpu.SemaphoreType.REGULAR((3,)),
        ],
        compiler_params=pltpu.CompilerParams(has_side_effects=True, collective_id=0, vmem_limit_bytes=56_000_000),
    )(layer_input, output_cot, hidden_cot, hidden_act, lengths)


def local(
    layer_input, output_cot, hidden_act, hidden_cot, lengths, weights, moment_one, moment_two
):
    by_place = (4, 4, 2, ROWS, SLOT)
    gradient, clip = exchange(
        layer_input, output_cot, hidden_cot.reshape(by_place), hidden_act.reshape(by_place), lengths.reshape(1, 32)
    )
    new_moment_one = beta_one * moment_one + (1.0 - beta_one) * gradient
    new_moment_two = beta_two * moment_two + (1.0 - beta_two) * gradient * gradient
    corr_one = 1.0 - beta_one**STEP
    corr_two = 1.0 - beta_two**STEP
    direction = new_moment_one / corr_one / (jnp.sqrt(new_moment_two / corr_two) + adam_eps)
    new_weights = weights - learn_rate * (direction + weight_decay * weights)
    return (new_weights, new_moment_one, new_moment_two, clip.reshape(32))


def solution(mesh):
    return jax.shard_map(
        local,
        mesh=mesh,
        in_specs=(
            P(("dp", "mp"), None, None),
            P(("dp", "mp"), None, None),
            P("dp", "mp", None),
            P("dp", "mp", None),
            P("dp"),
            P("dp", "mp"),
            P("dp", "mp"),
            P("dp", "mp"),
        ),
        out_specs=(P("dp", "mp"), P("dp", "mp"), P("dp", "mp"), P("dp")),
        check_vma=False,
    )
```
